512 devices in a mesh: groups: 2 (over y), blk: 64 (over z, core), head: 4 (over x).
Axes of the slice: x: 4, y: 2, z: 32, core: 2. Of those that a mesh axis runs over, the one named last changes fastest.
The devices are a block of a 4x8x32 slice.
Arguments:
- queries: bfloat16 [4, 64, 8192], P('groups', 'blk', 'head'), parts along dimension 0, may hold values from -4.5 to 4.5
- stored_cache_keys: bfloat16 [4, 32768, 1024], P('groups', 'blk', 'head'), parts along dimension 0, may hold values from -4.5 to 4.5
- stored_cache_values: bfloat16 [4, 32768, 1024], P('groups', 'blk', 'head'), parts along dimension 0, may hold values from -6 to 6
- out_weight: bfloat16 [8192, 8192], P('head', 'blk'), may hold values from -3 to 3
- lengths: int32 [4], P('groups'), parts along dimension 0, may hold values from 16384 to 32768
Outputs:
- projected: bfloat16 [4, 64, 8192], P('groups', 'head', 'blk'), parts along dimension 0
The draws below stay inside these ranges and needn't reach their ends.
There are 2 independent parts, one for each index of `groups`. The reference program is written for one: setup_inputs(seed, part) draws one part's arguments, and reference() takes and returns one part's arrays. A program takes and returns all parts, laid end to end along the dimension named above; an argument that names none is the same for every part. Nothing has to cross between parts.
All inputs are finite; a program needn't handle non-finite values.
Results may differ from the reference program's by a relative error of at most 0.0056.
Values may be sent and summed in bfloat16 or wider, within the bound.
No kernel may reach another device: no remote copies, remote signals or barrier semaphores. Data moves between devices by JAX's collectives and lax.ppermute only.
A program may use at most 64 MiB of HBM per device.

```python
import math
import jax
import jax.numpy as jnp
from jax import lax

REQUEST_COUNT = 2
QUERY_HEAD_COUNT = 64
KEY_VALUE_HEADS = 8
HEAD_DIMENSION = 128
D = 8192
CONTEXT_PER_BLOCK = 512
NEW_TOKENS = 64
CONTEXT_SIZE = 32768
N_BLK = 64


def draw_queries(key, part):
    base_offset = jnp.clip(jax.random.normal(jax.random.fold_in(key, 10), (REQUEST_COUNT, NEW_TOKENS, QUERY_HEAD_COUNT * HEAD_DIMENSION), jnp.float32), -4.5, 4.5)
    return base_offset.astype(jnp.bfloat16)


def draw_stored_cache_keys(key, part):
    base_offset = jnp.clip(jax.random.normal(jax.random.fold_in(key, 11), (REQUEST_COUNT, CONTEXT_SIZE, KEY_VALUE_HEADS * HEAD_DIMENSION), jnp.float32), -4.5, 4.5)
    return base_offset.astype(jnp.bfloat16)


def levels(rng, shape, shards, smallest, high):
    def one(dim, blocks):
        steps = jax.random.uniform(jax.random.fold_in(jax.random.fold_in(rng, 6), dim), (blocks,), jnp.float32, smallest / len(shards), high / len(shards))
        return jnp.repeat(jnp.exp(steps), shape[dim] // blocks).reshape((-1,) + (1,) * (len(shape) - dim - 1))

    gain = one(*shards[0])
    for cut in shards[1:]:
        gain = gain * one(*cut)
    return gain


def gaussian(rng, dims, width, bound, shards=(), kind=jnp.bfloat16):
    gain = levels(rng, dims, shards, -0.22, 0.18) if shards else 1.0
    result = jax.random.normal(rng, dims, jnp.float32) * width * gain
    return jnp.minimum(jnp.maximum(result, -bound), bound).astype(kind)


def setup_inputs(seed: int = 0, part: int = 0) -> dict:
    splits = jax.random.split(jax.random.key(seed), 6)
    own_keys = jax.random.split(jax.random.fold_in(splits[5], part), 6)
    return {
        "queries": draw_queries(jax.random.fold_in(jax.random.fold_in(splits[5], part), 71), part),
        "stored_cache_keys": draw_stored_cache_keys(jax.random.fold_in(jax.random.fold_in(splits[5], part), 71), part),
        "stored_cache_values": gaussian(own_keys[2], (REQUEST_COUNT, CONTEXT_SIZE, KEY_VALUE_HEADS * HEAD_DIMENSION), 1.0, 6.0, ((1, 64), (2, 4))),
        "out_weight": gaussian(splits[3], (QUERY_HEAD_COUNT * HEAD_DIMENSION, D), 0.5, 3.0, ((0, 4), (1, 64))),
        "lengths": jax.random.randint(own_keys[4], (REQUEST_COUNT,), CONTEXT_SIZE // 2, CONTEXT_SIZE + 1).astype(jnp.int32),
    }


masked_fill_value = -1e+30

def reference(queries, stored_cache_keys, stored_cache_values, out_weight, lengths):
    group_width = QUERY_HEAD_COUNT // KEY_VALUE_HEADS
    score_scale = 1.0 / math.sqrt(HEAD_DIMENSION)
    query_float = queries.astype(jnp.float32).reshape(REQUEST_COUNT, NEW_TOKENS, KEY_VALUE_HEADS, group_width, HEAD_DIMENSION)
    query_pos = lengths[:, None] - NEW_TOKENS + jnp.arange(NEW_TOKENS, dtype=jnp.int32)[None, :]

    def advance(carry, block):
        run_max, run_total, run_sum = carry
        first_position = (block * CONTEXT_PER_BLOCK).astype(jnp.int32)
        local_keys = lax.dynamic_slice_in_dim(stored_cache_keys, first_position, CONTEXT_PER_BLOCK, 1).astype(jnp.float32).reshape(REQUEST_COUNT, CONTEXT_PER_BLOCK, KEY_VALUE_HEADS, HEAD_DIMENSION)
        local_values = lax.dynamic_slice_in_dim(stored_cache_values, first_position, CONTEXT_PER_BLOCK, 1).astype(jnp.float32).reshape(REQUEST_COUNT, CONTEXT_PER_BLOCK, KEY_VALUE_HEADS, HEAD_DIMENSION)
        scores = jnp.einsum('rnkgd,rckd->rnkgc', query_float, local_keys) * score_scale
        key_pos = first_position + jnp.arange(CONTEXT_PER_BLOCK, dtype=jnp.int32)
        visible = (key_pos[None, None, :] <= query_pos[:, :, None])[:, :, None, None, :]
        block_max = lax.optimization_barrier(jnp.max(jnp.where(visible, scores, masked_fill_value), axis=-1))
        weights = jnp.where(visible, jnp.exp(scores - block_max[..., None]), 0.0)
        block_total = lax.optimization_barrier(jnp.sum(weights, axis=-1))
        rounded = lax.optimization_barrier(weights.astype(jnp.bfloat16)).astype(jnp.float32)
        block_sum = jnp.einsum('rnkgc,rckd->rnkgd', rounded, local_values)
        new_max = jnp.maximum(run_max, block_max)
        old_factor = jnp.exp(run_max - new_max)
        new_factor = jnp.exp(block_max - new_max)
        run_total = run_total * old_factor + block_total * new_factor
        run_sum = run_sum * old_factor[..., None] + block_sum * new_factor[..., None]
        return ((new_max, run_total, run_sum), None)
    initial_state = (jnp.full((REQUEST_COUNT, NEW_TOKENS, KEY_VALUE_HEADS, group_width), masked_fill_value, jnp.float32), jnp.zeros((REQUEST_COUNT, NEW_TOKENS, KEY_VALUE_HEADS, group_width), jnp.float32), jnp.zeros((REQUEST_COUNT, NEW_TOKENS, KEY_VALUE_HEADS, group_width, HEAD_DIMENSION), jnp.float32))
    final, _ = lax.scan(advance, initial_state, jnp.arange(N_BLK, dtype=jnp.int32))
    run_max, run_total, run_sum = final
    attention = (run_sum / run_total[..., None]).astype(jnp.bfloat16).reshape(REQUEST_COUNT * NEW_TOKENS, QUERY_HEAD_COUNT * HEAD_DIMENSION)
    output = jnp.dot(attention, out_weight, preferred_element_type=jnp.float32)
    return output.astype(jnp.bfloat16).reshape(REQUEST_COUNT, NEW_TOKENS, D)
```

```python
import functools
import math

import jax
import jax.numpy as jnp
from jax import lax
from jax.experimental import pallas as pl
from jax.experimental.pallas import tpu as pltpu
from jax.sharding import Mesh
from jax.sharding import PartitionSpec as P

KEY_VALUE_HEADS = 8
HEAD_DIMENSION = 128
CORES = 2
BLK = ("z", "core")

masked_fill_value = -1e30
bf16 = jnp.bfloat16
f32 = jnp.float32


def attention_kernel(place, lengths, queries, own_keys, own_values, other_keys, other_values, out):
    new_count, requests, group, dim = queries.shape
    homes, per_home = out.shape[0], new_count // out.shape[0]
    span = own_keys.shape[1]
    rows = new_count * group
    kept = per_home * requests
    scale = 1.0 / math.sqrt(dim)
    lane = lax.broadcasted_iota(jnp.int32, (homes, group, dim), 2)
    stats = jnp.zeros((homes, group, dim), f32)
    token = lax.broadcasted_iota(jnp.int32, (rows, span), 0) // group
    column = lax.broadcasted_iota(jnp.int32, (rows, span), 1)
    for r in range(requests):
        q = queries[:, r].astype(f32).reshape(rows, dim).astype(bf16)
        last = lengths[r] - new_count
        keys = (own_keys[r], other_keys[pl.ds(r * span, span), :])
        values = (own_values[r], other_values[pl.ds(r * span, span), :])
        scores, seen = [], []
        top = None
        for part in range(2):
            s = lax.dot_general(q, keys[part], (((1,), (1,)), ((), ())), preferred_element_type=f32) * scale
            visible = column - token <= last - place[1 + part]
            s = jnp.where(visible, s, masked_fill_value)
            m = jnp.max(s, axis=1, keepdims=True)
            top = m if top is None else jnp.maximum(top, m)
            scores.append(s)
            seen.append(visible)
        shift = top.astype(bf16).astype(f32)
        total, summed = None, None
        for part in range(2):
            w = jnp.where(seen[part], jnp.exp(scores[part] - shift), 0.0)
            t = jnp.sum(w, axis=1, keepdims=True)
            o = jnp.dot(w.astype(bf16), values[part], preferred_element_type=f32)
            total = t if total is None else total + t
            summed = o if summed is None else summed + o
        high = total.astype(bf16).astype(f32)
        low = total - high
        summed = summed.reshape(homes, per_home, group, dim)
        for t in range(per_home):
            k = t * requests + r
            out[:, k] = summed[:, t].astype(bf16)
            for j, v in enumerate((shift, high, low)):
                v = v.reshape(homes, per_home, group, 1)[:, t]
                stats = jnp.where(lane == j * kept + k, v, stats)
    out[:, kept] = stats.astype(bf16)


def merge_kernel(parts, out):
    blocks, kept, dim = parts.shape[0], parts.shape[1] - 1, parts.shape[3]
    stats = parts[:, kept].astype(f32)
    factor = jnp.exp(stats - jnp.max(stats, axis=0, keepdims=True))
    group = stats.shape[1]
    flat = stats.reshape(blocks * group, dim)
    total = pltpu.roll(flat, dim - kept, 1) + pltpu.roll(flat, dim - 2 * kept, 1)
    total = jnp.sum(factor * total.reshape(stats.shape), axis=0)
    for k in range(kept):
        summed = jnp.sum(parts[:, k].astype(f32) * factor[:, :, k : k + 1], axis=0)
        row = (summed / total[:, k : k + 1]).astype(bf16)
        out[:, k] = jnp.broadcast_to(row[None], (blocks, group, dim))


def body(queries, stored_cache_keys, stored_cache_values, out_weight, lengths):
    requests, span, _ = stored_cache_keys.shape
    z_count, x_count = lax.axis_size("z"), lax.axis_size("head")
    new_count = queries.shape[1] * z_count * CORES
    dim = HEAD_DIMENSION
    group = queries.shape[2] // (CORES * dim)
    inputs = out_weight.shape[0] // CORES
    columns = out_weight.shape[1]
    z, core = lax.axis_index("z"), lax.axis_index("core")
    per_home = new_count // z_count
    kept = per_home * requests

    def head_of(cache, which):
        return lax.dynamic_slice_in_dim(cache, which * dim, dim, 2).reshape(requests * span, dim)

    leaving = jnp.concatenate(
        [
            head_of(stored_cache_keys, 1 - core),
            head_of(stored_cache_values, 1 - core),
            lax.dynamic_slice_in_dim(out_weight, (1 - core) * inputs, inputs, 0),
        ],
        axis=0,
    )
    arrived = lax.ppermute(leaving, "core", [(0, 1), (1, 0)])

    pieces = queries.reshape(requests, CORES, group, dim).transpose(1, 0, 2, 3)
    pieces = jnp.broadcast_to(pieces[None], (z_count, *pieces.shape)).reshape(-1, *pieces.shape[1:])
    all_queries = lax.all_to_all(pieces, BLK, 0, 0, tiled=True)

    place = jnp.stack([core, (z * CORES + core) * span, (z * CORES + 1 - core) * span]).astype(jnp.int32)
    rest = requests * span
    whole = lambda *shape: pl.BlockSpec(shape, lambda i, p, n: (0,) * len(shape))
    cache = pl.BlockSpec((requests, span, dim), lambda i, p, n: (0, 0, p[0]))
    partial = pl.pallas_call(
        attention_kernel,
        grid_spec=pltpu.PrefetchScalarGridSpec(
            num_scalar_prefetch=2,
            grid=(1,),
            in_specs=[
                whole(*all_queries.shape),
                cache,
                cache,
                pl.BlockSpec((rest, dim), lambda i, p, n: (0, 0)),
                pl.BlockSpec((rest, dim), lambda i, p, n: (1, 0)),
            ],
            out_specs=whole(z_count, kept + 1, group, dim),
        ),
        out_shape=jax.ShapeDtypeStruct((z_count, kept + 1, group, dim), bf16),
        name="attention",
    )(place, lengths, all_queries, stored_cache_keys, stored_cache_values, arrived, arrived)

    parts = lax.all_to_all(partial, "z", 0, 0, tiled=True)
    own = pl.pallas_call(
        merge_kernel,
        out_shape=jax.ShapeDtypeStruct((z_count, kept, group, dim), bf16),
        name="merge",
    )(parts)
    attention = lax.all_to_all(own, "z", 0, 0, tiled=True)

    mine = lax.dynamic_slice_in_dim(out_weight, core * inputs, inputs, 0)
    theirs = arrived[2 * rest :]
    first = core == 0
    weight = jnp.concatenate([jnp.where(first, mine, theirs), jnp.where(first, theirs, mine)], axis=1)
    terms = jnp.dot(
        attention.reshape(z_count * kept, group * dim), weight, preferred_element_type=f32
    )
    terms = terms.reshape(x_count, -1, CORES, columns).transpose(0, 2, 1, 3)
    terms = terms.reshape(x_count * CORES, -1, columns)
    terms = lax.all_to_all(terms, ("head", "core"), 0, 0, tiled=True).sum(axis=0)
    terms = terms.reshape(-1, requests, columns).transpose(1, 0, 2)
    return terms.astype(bf16)


def solution(mesh):
    shape = mesh.devices.shape
    torus = Mesh(
        mesh.devices.reshape(shape[0], shape[1] // CORES, CORES, shape[2]),
        ("groups", "z", "core", "head"),
    )
    return jax.shard_map(
        body,
        mesh=torus,
        in_specs=(
            P("groups", BLK, "head"),
            P("groups", BLK, "head"),
            P("groups", BLK, "head"),
            P("head", BLK),
            P("groups"),
        ),
        out_specs=P("groups", "head", BLK),
        check_vma=False,
    )
```

```python
import functools
import math

import jax
import jax.numpy as jnp
from jax import lax
from jax.experimental import pallas as pl
from jax.experimental.pallas import tpu as pltpu
from jax.sharding import Mesh
from jax.sharding import PartitionSpec as P

KEY_VALUE_HEADS = 8
HEAD_DIMENSION = 128
CORES = 2
BLK = ("z", "core")

masked_fill_value = -1e30
bf16 = jnp.bfloat16
f32 = jnp.float32


def attention_kernel(place, lengths, queries, own_keys, own_values, other_keys, other_values, out):
    new_count, requests, group, dim = queries.shape
    homes, per_home = out.shape[0], new_count // out.shape[0]
    span = own_keys.shape[1]
    rows = new_count * group
    kept = per_home * requests
    scale = 1.0 / math.sqrt(dim)
    lane = lax.broadcasted_iota(jnp.int32, (homes, group, dim), 2)
    stats = jnp.zeros((homes, group, dim), f32)
    token = lax.broadcasted_iota(jnp.int32, (rows, span), 0) // group
    column = lax.broadcasted_iota(jnp.int32, (rows, span), 1)
    for r in range(requests):
        q = queries[:, r].astype(f32).reshape(rows, dim).astype(bf16)
        last = lengths[r] - new_count
        keys = (own_keys[r], other_keys[pl.ds(r * span, span), :])
        values = (own_values[r], other_values[pl.ds(r * span, span), :])
        scores, seen = [], []
        top = None
        for part in range(2):
            s = lax.dot_general(q, keys[part], (((1,), (1,)), ((), ())), preferred_element_type=f32) * scale
            visible = column - token <= last - place[1 + part]
            s = jnp.where(visible, s, masked_fill_value)
            m = jnp.max(s, axis=1, keepdims=True)
            top = m if top is None else jnp.maximum(top, m)
            scores.append(s)
            seen.append(visible)
        shift = top.astype(bf16).astype(f32)
        total, summed = None, None
        for part in range(2):
            w = jnp.where(seen[part], jnp.exp(scores[part] - shift), 0.0)
            t = jnp.sum(w, axis=1, keepdims=True)
            o = jnp.dot(w.astype(bf16), values[part], preferred_element_type=f32)
            total = t if total is None else total + t
            summed = o if summed is None else summed + o
        high = total.astype(bf16).astype(f32)
        low = total - high
        summed = summed.reshape(homes, per_home, group, dim)
        for t in range(per_home):
            k = t * requests + r
            out[:, k] = summed[:, t].astype(bf16)
            for j, v in enumerate((shift, high, low)):
                v = v.reshape(homes, per_home, group, 1)[:, t]
                stats = jnp.where(lane == j * kept + k, v, stats)
    out[:, kept] = stats.astype(bf16)


def merge_kernel(parts, out):
    blocks, kept, dim = parts.shape[0], parts.shape[1] - 1, parts.shape[3]
    stats = parts[:, kept].astype(f32)
    factor = jnp.exp(stats - jnp.max(stats, axis=0, keepdims=True))
    group = stats.shape[1]
    flat = stats.reshape(blocks * group, dim)
    total = pltpu.roll(flat, dim - kept, 1) + pltpu.roll(flat, dim - 2 * kept, 1)
    total = jnp.sum(factor * total.reshape(stats.shape), axis=0)
    for k in range(kept):
        summed = jnp.sum(parts[:, k].astype(f32) * factor[:, :, k : k + 1], axis=0)
        row = (summed / total[:, k : k + 1]).astype(bf16)
        out[:, k] = jnp.broadcast_to(row[None], (blocks, group, dim))


def project_kernel(place, attention, mine, theirs, out, wide):
    pieces, per_piece, columns = out.shape
    inputs, dim = mine.shape[0], attention.shape[1]
    group = inputs // dim
    rows = attention.shape[0] // group
    wide[...] = attention[...].astype(f32)
    left = jnp.concatenate(
        [wide[pl.ds(h, rows, stride=group), :].astype(bf16) for h in range(group)], axis=1
    )
    for weight, core in ((mine, place[0]), (theirs, 1 - place[0])):
        terms = jnp.dot(left, weight[...], preferred_element_type=f32)
        for x in range(pieces // CORES):
            out[x * CORES + core] = terms[x * per_piece : (x + 1) * per_piece]


def body(queries, stored_cache_keys, stored_cache_values, out_weight, lengths):
    requests, span, _ = stored_cache_keys.shape
    z_count, x_count = lax.axis_size("z"), lax.axis_size("head")
    new_count = queries.shape[1] * z_count * CORES
    dim = HEAD_DIMENSION
    group = queries.shape[2] // (CORES * dim)
    inputs = out_weight.shape[0] // CORES
    columns = out_weight.shape[1]
    z, core = lax.axis_index("z"), lax.axis_index("core")
    per_home = new_count // z_count
    kept = per_home * requests

    def head_of(cache, which):
        return lax.dynamic_slice_in_dim(cache, which * dim, dim, 2).reshape(requests * span, dim)

    leaving = jnp.concatenate(
        [
            head_of(stored_cache_keys, 1 - core),
            head_of(stored_cache_values, 1 - core),
            lax.dynamic_slice_in_dim(out_weight, (1 - core) * inputs, inputs, 0),
        ],
        axis=0,
    )
    arrived = lax.ppermute(leaving, "core", [(0, 1), (1, 0)])

    pieces = queries.reshape(requests, CORES, group, dim).transpose(1, 0, 2, 3)
    pieces = jnp.broadcast_to(pieces[None], (z_count, *pieces.shape)).reshape(-1, *pieces.shape[1:])
    place = jnp.stack([core, (z * CORES + core) * span, (z * CORES + 1 - core) * span]).astype(jnp.int32)
    pieces, place, _ = lax.optimization_barrier((pieces, place, arrived))
    all_queries = lax.all_to_all(pieces, BLK, 0, 0, tiled=True)

    rest = requests * span
    whole = lambda *shape: pl.BlockSpec(shape, lambda i, p, n: (0,) * len(shape))
    cache = pl.BlockSpec((requests, span, dim), lambda i, p, n: (0, 0, p[0]))
    partial = pl.pallas_call(
        attention_kernel,
        grid_spec=pltpu.PrefetchScalarGridSpec(
            num_scalar_prefetch=2,
            grid=(1,),
            in_specs=[
                whole(*all_queries.shape),
                cache,
                cache,
                pl.BlockSpec((rest, dim), lambda i, p, n: (0, 0)),
                pl.BlockSpec((rest, dim), lambda i, p, n: (1, 0)),
            ],
            out_specs=whole(z_count, kept + 1, group, dim),
        ),
        out_shape=jax.ShapeDtypeStruct((z_count, kept + 1, group, dim), bf16),
        name="attention",
    )(place, lengths, all_queries, stored_cache_keys, stored_cache_values, arrived, arrived)

    parts = lax.all_to_all(partial, "z", 0, 0, tiled=True)
    own = pl.pallas_call(
        merge_kernel,
        out_shape=jax.ShapeDtypeStruct((z_count, kept, group, dim), bf16),
        name="merge",
    )(parts)
    attention = lax.all_to_all(own, "z", 0, 0, tiled=True)

    rows = z_count * kept
    terms = pl.pallas_call(
        project_kernel,
        grid_spec=pltpu.PrefetchScalarGridSpec(
            num_scalar_prefetch=1,
            grid=(1,),
            in_specs=[
                pl.BlockSpec((rows * group, dim), lambda i, p: (0, 0)),
                pl.BlockSpec((inputs, columns), lambda i, p: (p[0], 0)),
                pl.BlockSpec((inputs, columns), lambda i, p: (2 * rest // inputs, 0)),
            ],
            out_specs=pl.BlockSpec((x_count * CORES, rows // x_count, columns), lambda i, p: (0, 0, 0)),
            scratch_shapes=[pltpu.VMEM((rows * group, dim), f32)],
        ),
        out_shape=jax.ShapeDtypeStruct((x_count * CORES, rows // x_count, columns), f32),
        name="project",
    )(place, attention.reshape(rows * group, dim), out_weight, arrived)
    terms = lax.all_to_all(terms, ("head", "core"), 0, 0, tiled=True).sum(axis=0)
    terms = terms.reshape(-1, requests, columns).transpose(1, 0, 2)
    return terms.astype(bf16)


def solution(mesh):
    shape = mesh.devices.shape
    torus = Mesh(
        mesh.devices.reshape(shape[0], shape[1] // CORES, CORES, shape[2]),
        ("groups", "z", "core", "head"),
    )
    return jax.shard_map(
        body,
        mesh=torus,
        in_specs=(
            P("groups", BLK, "head"),
            P("groups", BLK, "head"),
            P("groups", BLK, "head"),
            P("head", BLK),
            P("groups"),
        ),
        out_specs=P("groups", "head", BLK),
        check_vma=False,
    )
```

```python
import math

import jax
import jax.numpy as jnp
from jax import lax
from jax.experimental import pallas as pl
from jax.experimental.pallas import tpu as pltpu
from jax.sharding import Mesh
from jax.sharding import PartitionSpec as P

KEY_VALUE_HEADS = 8
HEAD_DIMENSION = 128
CORES = 2
BLK = ("z", "core")

masked_fill_value = -1e30
bf16 = jnp.bfloat16
f32 = jnp.float32


def in_vmem(kernel, name, shape, dtype, **more):
    def call(*arrays):
        scalar = [a.dtype == jnp.int32 for a in arrays]
        return pl.pallas_call(
            kernel,
            in_specs=[pl.BlockSpec(memory_space=pltpu.SMEM if s else pltpu.VMEM) for s in scalar],
            out_specs=pl.BlockSpec(memory_space=pltpu.VMEM),
            out_shape=pltpu.VMEM(shape, dtype),
            name=name,
            **more,
        )(*(a if s else pltpu.with_memory_space_constraint(a, pltpu.VMEM) for a, s in zip(arrays, scalar)))

    return call


def attention_kernel(place, lengths, queries, own_keys, own_values, other, out):
    new_count, requests, group, dim = queries.shape
    homes, per_home = out.shape[0], new_count // out.shape[0]
    span = own_keys.shape[1]
    rows = new_count * group
    kept = per_home * requests
    scale = 1.0 / math.sqrt(dim)
    head = pl.ds(pl.multiple_of(place[0] * dim, dim), dim)
    lane = lax.broadcasted_iota(jnp.int32, (homes, group, dim), 2)
    stats = jnp.zeros((homes, group, dim), f32)
    token = lax.broadcasted_iota(jnp.int32, (rows, span), 0) // group
    column = lax.broadcasted_iota(jnp.int32, (rows, span), 1)
    for r in range(requests):
        q = queries[:, r].astype(f32).reshape(rows, dim).astype(bf16)
        last = lengths[r] - new_count
        keys = (own_keys[r, :, head], other[pl.ds(r * span, span), :])
        values = (own_values[r, :, head], other[pl.ds((requests + r) * span, span), :])
        scores, seen = [], []
        top = None
        for part in range(2):
            s = lax.dot_general(q, keys[part], (((1,), (1,)), ((), ())), preferred_element_type=f32) * scale
            visible = column - token <= last - place[1 + part]
            s = jnp.where(visible, s, masked_fill_value)
            m = jnp.max(s, axis=1, keepdims=True)
            top = m if top is None else jnp.maximum(top, m)
            scores.append(s)
            seen.append(visible)
        shift = top.astype(bf16).astype(f32)
        total, summed = None, None
        for part in range(2):
            w = jnp.where(seen[part], jnp.exp(scores[part] - shift), 0.0)
            t = jnp.sum(w, axis=1, keepdims=True)
            o = jnp.dot(w.astype(bf16), values[part], preferred_element_type=f32)
            total = t if total is None else total + t
            summed = o if summed is None else summed + o
        high = total.astype(bf16).astype(f32)
        low = total - high
        summed = summed.reshape(homes, per_home, group, dim)
        for t in range(per_home):
            k = t * requests + r
            out[:, k] = summed[:, t].astype(bf16)
            for j, v in enumerate((shift, high, low)):
                v = v.reshape(homes, per_home, group, 1)[:, t]
                stats = jnp.where(lane == j * kept + k, v, stats)
    out[:, kept] = stats.astype(bf16)


def merge_kernel(parts, out):
    blocks, kept, dim = parts.shape[0], parts.shape[1] - 1, parts.shape[3]
    stats = parts[:, kept].astype(f32)
    factor = jnp.exp(stats - jnp.max(stats, axis=0, keepdims=True))
    group = stats.shape[1]
    flat = stats.reshape(blocks * group, dim)
    total = pltpu.roll(flat, dim - kept, 1) + pltpu.roll(flat, dim - 2 * kept, 1)
    total = jnp.sum(factor * total.reshape(stats.shape), axis=0)
    for k in range(kept):
        summed = jnp.sum(parts[:, k].astype(f32) * factor[:, :, k : k + 1], axis=0)
        row = (summed / total[:, k : k + 1]).astype(bf16)
        out[:, k] = jnp.broadcast_to(row[None], (blocks, group, dim))


def project_kernel(place, attention, weight, other, out, wide):
    pieces, per_piece, columns = out.shape
    inputs, dim = weight.shape[0] // CORES, attention.shape[1]
    group = inputs // dim
    rows = attention.shape[0] // group
    wide[...] = attention[...].astype(f32)
    left = jnp.concatenate(
        [wide[pl.ds(h, rows, stride=group), :].astype(bf16) for h in range(group)], axis=1
    )
    mine = weight[pl.ds(pl.multiple_of(place[0] * inputs, inputs), inputs), :]
    theirs = other[other.shape[0] - inputs :, :]
    for right, core in ((mine, place[0]), (theirs, 1 - place[0])):
        terms = jnp.dot(left, right, preferred_element_type=f32)
        for x in range(pieces // CORES):
            out[x * CORES + core] = terms[x * per_piece : (x + 1) * per_piece]


def body(queries, stored_cache_keys, stored_cache_values, out_weight, lengths):
    requests, span, _ = stored_cache_keys.shape
    z_count, x_count = lax.axis_size("z"), lax.axis_size("head")
    new_count = queries.shape[1] * z_count * CORES
    dim = HEAD_DIMENSION
    group = queries.shape[2] // (CORES * dim)
    inputs = out_weight.shape[0] // CORES
    columns = out_weight.shape[1]
    z, core = lax.axis_index("z"), lax.axis_index("core")
    per_home = new_count // z_count
    kept = per_home * requests

    def head_of(cache, which):
        return lax.dynamic_slice_in_dim(cache, which * dim, dim, 2).reshape(requests * span, dim)

    leaving = jnp.concatenate(
        [
            head_of(stored_cache_keys, 1 - core),
            head_of(stored_cache_values, 1 - core),
            lax.dynamic_slice_in_dim(out_weight, (1 - core) * inputs, inputs, 0),
        ],
        axis=0,
    )
    arrived = lax.ppermute(leaving, "core", [(0, 1), (1, 0)])

    pieces = queries.reshape(requests, CORES, group, dim).transpose(1, 0, 2, 3)
    pieces = jnp.broadcast_to(pieces[None], (z_count, *pieces.shape)).reshape(-1, *pieces.shape[1:])
    place = jnp.stack([core, (z * CORES + core) * span, (z * CORES + 1 - core) * span]).astype(jnp.int32)
    all_queries = lax.all_to_all(pieces, BLK, 0, 0, tiled=True)

    partial = in_vmem(attention_kernel, "attention", (z_count, kept + 1, group, dim), bf16)(
        place, lengths, all_queries, stored_cache_keys, stored_cache_values, arrived
    )

    parts = lax.all_to_all(partial, "z", 0, 0, tiled=True)
    own = in_vmem(merge_kernel, "merge", (z_count, kept, group, dim), bf16)(parts)
    attention = lax.all_to_all(own, "z", 0, 0, tiled=True)

    rows = z_count * kept
    terms = in_vmem(
        project_kernel,
        "project",
        (x_count * CORES, rows // x_count, columns),
        f32,
        scratch_shapes=[pltpu.VMEM((rows * group, dim), f32)],
    )(place, attention.reshape(rows * group, dim), out_weight, arrived)
    terms = lax.all_to_all(terms, ("head", "core"), 0, 0, tiled=True).sum(axis=0)
    terms = terms.reshape(-1, requests, columns).transpose(1, 0, 2)
    return terms.astype(bf16)


def solution(mesh):
    shape = mesh.devices.shape
    torus = Mesh(
        mesh.devices.reshape(shape[0], shape[1] // CORES, CORES, shape[2]),
        ("groups", "z", "core", "head"),
    )
    return jax.shard_map(
        body,
        mesh=torus,
        in_specs=(
            P("groups", BLK, "head"),
            P("groups", BLK, "head"),
            P("groups", BLK, "head"),
            P("head", BLK),
            P("groups"),
        ),
        out_specs=P("groups", "head", BLK),
        check_vma=False,
    )
```

```python
import functools
import math

import jax
import jax.numpy as jnp
from jax import lax
from jax.experimental import pallas as pl
from jax.experimental.pallas import tpu as pltpu
from jax.sharding import Mesh
from jax.sharding import PartitionSpec as P

KEY_VALUE_HEADS = 8
HEAD_DIMENSION = 128
CORES = 2
BLK = ("far", "near", "core")
NEAR = 4

masked_fill_value = -1e30
bf16 = jnp.bfloat16
f32 = jnp.float32


def in_vmem(kernel, name, shape, dtype, **more):
    def call(*arrays):
        scalar = [a.dtype == jnp.int32 for a in arrays]
        return pl.pallas_call(
            kernel,
            in_specs=[pl.BlockSpec(memory_space=pltpu.SMEM if s else pltpu.VMEM) for s in scalar],
            out_specs=pl.BlockSpec(memory_space=pltpu.VMEM),
            out_shape=pltpu.VMEM(shape, dtype),
            name=name,
            **more,
        )(*(a if s else pltpu.with_memory_space_constraint(a, pltpu.VMEM) for a, s in zip(arrays, scalar)))

    return call


def attention_kernel(place, lengths, queries, own_keys, own_values, other, out):
    new_count, requests, group, dim = queries.shape
    homes, per_home = out.shape[0], new_count // out.shape[0]
    span = own_keys.shape[1]
    rows = new_count * group
    far = homes // NEAR
    kept = per_home * requests
    scale = 1.0 / math.sqrt(dim)
    head = pl.ds(pl.multiple_of(place[0] * dim, dim), dim)
    lane = lax.broadcasted_iota(jnp.int32, (homes, group, dim), 2)
    stats = jnp.zeros((homes, group, dim), f32)
    home = lax.broadcasted_iota(jnp.int32, (rows, span), 0) // (group * per_home)
    token = (home % far * NEAR + home // far) * per_home
    token += lax.broadcasted_iota(jnp.int32, (rows, span), 0) // group % per_home
    column = lax.broadcasted_iota(jnp.int32, (rows, span), 1)
    for r in range(requests):
        q = queries[:, r].astype(f32).reshape(rows, dim).astype(bf16)
        last = lengths[r] - new_count
        keys = (own_keys[r, :, head], other[pl.ds(r * span, span), :])
        values = (own_values[r, :, head], other[pl.ds((requests + r) * span, span), :])
        scores, seen = [], []
        top = None
        for part in range(2):
            s = lax.dot_general(q, keys[part], (((1,), (1,)), ((), ())), preferred_element_type=f32) * scale
            visible = column - token <= last - place[1 + part]
            s = jnp.where(visible, s, masked_fill_value)
            m = jnp.max(s, axis=1, keepdims=True)
            top = m if top is None else jnp.maximum(top, m)
            scores.append(s)
            seen.append(visible)
        shift = top.astype(bf16).astype(f32)
        total, summed = None, None
        for part in range(2):
            w = jnp.where(seen[part], jnp.exp(scores[part] - shift), 0.0)
            t = jnp.sum(w, axis=1, keepdims=True)
            o = jnp.dot(w.astype(bf16), values[part], preferred_element_type=f32)
            total = t if total is None else total + t
            summed = o if summed is None else summed + o
        high = total.astype(bf16).astype(f32)
        low = total - high
        summed = summed.reshape(homes, per_home, group, dim)
        for t in range(per_home):
            k = t * requests + r
            out[:, k] = summed[:, t].astype(bf16)
            for j, v in enumerate((shift, high, low)):
                v = v.reshape(homes, per_home, group, 1)[:, t]
                stats = jnp.where(lane == j * kept + k, v, stats)
    out[:, kept] = stats.astype(bf16)


def merged(parts):
    kept, group, dim = parts.shape[-3] - 1, parts.shape[-2], parts.shape[-1]
    stats = parts[..., kept, :, :].astype(f32)
    shift = jnp.max(stats, axis=0)
    factor = jnp.exp(stats - shift[None])
    flat = stats.reshape(-1, dim)
    total = pltpu.roll(flat, dim - kept, 1) + pltpu.roll(flat, dim - 2 * kept, 1)
    total = jnp.sum(factor * total.reshape(stats.shape), axis=0)
    rows = [
        jnp.sum(parts[..., k, :, :].astype(f32) * factor[..., k : k + 1], axis=0) for k in range(kept)
    ]
    return rows, shift, total


def merge_near_kernel(parts, out):
    kept, group, dim = parts.shape[-3] - 1, parts.shape[-2], parts.shape[-1]
    rows, shift, total = merged(parts)
    for k in range(kept):
        out[:, k] = rows[k].astype(bf16)
    high = total.astype(bf16).astype(f32)
    low = (total - high).reshape(-1, dim)
    high = pltpu.roll(high.reshape(-1, dim), kept, 1).reshape(shift.shape)
    low = pltpu.roll(low, 2 * kept, 1).reshape(shift.shape)
    lane = lax.broadcasted_iota(jnp.int32, shift.shape, len(shift.shape) - 1)
    out[:, kept] = jnp.where(lane < kept, shift, jnp.where(lane < 2 * kept, high, low)).astype(bf16)


def merge_far_kernel(parts, out):
    rows, _, total = merged(parts)
    for k, row in enumerate(rows):
        row = (row / total[:, k : k + 1]).astype(bf16)
        out[:, k] = jnp.broadcast_to(row[None], (out.shape[0], *row.shape))


def project_kernel(block, place, attention, weight, other, out, wide):
    pieces, per_piece, columns = out.shape
    inputs, dim = weight.shape[0] // CORES, attention.shape[1]
    group = inputs // dim
    rows = attention.shape[0] // group
    homes = wide.shape[0] // block
    for h in range(homes):
        source = h % NEAR * (homes // NEAR) + h // NEAR
        wide[h * block : (h + 1) * block] = attention[source * block : (source + 1) * block].astype(f32)
    left = jnp.concatenate(
        [wide[pl.ds(h, rows, stride=group), :].astype(bf16) for h in range(group)], axis=1
    )
    mine = weight[pl.ds(pl.multiple_of(place[0] * inputs, inputs), inputs), :]
    theirs = other[other.shape[0] - inputs :, :]
    for right, core in ((mine, place[0]), (theirs, 1 - place[0])):
        terms = jnp.dot(left, right, preferred_element_type=f32)
        for x in range(pieces // CORES):
            out[x * CORES + core] = terms[x * per_piece : (x + 1) * per_piece]


def exchanged(pieces, axes):
    flat = pieces.reshape(pieces.shape[0], -1, pieces.shape[-1])
    return lax.all_to_all(flat, axes, 0, 0, tiled=True).reshape(pieces.shape)


def shared(value, axis):
    return exchanged(jnp.broadcast_to(value[None], (lax.axis_size(axis), *value.shape)), axis)


def body(queries, stored_cache_keys, stored_cache_values, out_weight, lengths):
    requests, span, _ = stored_cache_keys.shape
    far_count, x_count = lax.axis_size("far"), lax.axis_size("head")
    z_count = far_count * NEAR
    new_count = queries.shape[1] * z_count * CORES
    dim = HEAD_DIMENSION
    group = queries.shape[2] // (CORES * dim)
    inputs = out_weight.shape[0] // CORES
    columns = out_weight.shape[1]
    z, core = lax.axis_index(("far", "near")), lax.axis_index("core")
    per_home = new_count // z_count
    kept = per_home * requests

    def head_of(cache, which):
        return lax.dynamic_slice_in_dim(cache, which * dim, dim, 2).reshape(requests * span, dim)

    leaving = jnp.concatenate(
        [
            head_of(stored_cache_keys, 1 - core),
            head_of(stored_cache_values, 1 - core),
            lax.dynamic_slice_in_dim(out_weight, (1 - core) * inputs, inputs, 0),
        ],
        axis=0,
    )
    arrived = lax.ppermute(leaving, "core", [(0, 1), (1, 0)])

    pieces = queries.reshape(requests, CORES, group, dim).transpose(1, 0, 2, 3)
    pieces = jnp.broadcast_to(pieces[None], (far_count, *pieces.shape)).reshape(-1, *pieces.shape[1:])
    all_queries = shared(exchanged(pieces, ("far", "core")), "near").reshape(new_count, requests, group, dim)

    place = jnp.stack([core, (z * CORES + core) * span, (z * CORES + 1 - core) * span]).astype(jnp.int32)

    partial = in_vmem(attention_kernel, "attention", (z_count, kept + 1, group, dim), bf16)(
        place, lengths, all_queries, stored_cache_keys, stored_cache_values, arrived
    )

    sent = partial.reshape(NEAR, far_count, *partial.shape[1:])
    partial = in_vmem(merge_near_kernel, "merge_near", sent.shape[1:], bf16)(exchanged(sent, "near"))
    own = in_vmem(merge_far_kernel, "merge_far", (far_count, kept, group, dim), bf16)(
        exchanged(partial, "far")
    )
    attention = shared(exchanged(own, "far"), "near")

    rows = z_count * kept
    terms = in_vmem(
        functools.partial(project_kernel, kept * group),
        "project",
        (x_count * CORES, rows // x_count, columns),
        f32,
        scratch_shapes=[pltpu.VMEM((rows * group, dim), f32)],
    )(place, attention.reshape(rows * group, dim), out_weight, arrived)
    terms = lax.all_to_all(terms, ("head", "core"), 0, 0, tiled=True).sum(axis=0)
    terms = terms.reshape(-1, requests, columns).transpose(1, 0, 2)
    return terms.astype(bf16)


def solution(mesh):
    shape = mesh.devices.shape
    torus = Mesh(
        mesh.devices.reshape(shape[0], -1, NEAR, CORES, shape[2]),
        ("groups", "far", "near", "core", "head"),
    )
    return jax.shard_map(
        body,
        mesh=torus,
        in_specs=(
            P("groups", BLK, "head"),
            P("groups", BLK, "head"),
            P("groups", BLK, "head"),
            P("head", BLK),
            P("groups"),
        ),
        out_specs=P("groups", "head", BLK),
        check_vma=False,
    )
```

```python
import functools
import math

import jax
import jax.numpy as jnp
from jax import lax
from jax.experimental import pallas as pl
from jax.experimental.pallas import tpu as pltpu
from jax.sharding import Mesh
from jax.sharding import PartitionSpec as P


HEAD_DIMENSION = 128
CORES = 2
BLK = ("far", "near", "core")
NEAR = 4

masked_fill_value = -1e30
bf16 = jnp.bfloat16
f32 = jnp.float32


def in_vmem(kernel, shape, dtype, **more):
    def call(*arrays):
        scalar = [a.dtype == jnp.int32 for a in arrays]
        return pl.pallas_call(
            kernel,
            in_specs=[pl.BlockSpec(memory_space=pltpu.SMEM if s else pltpu.VMEM) for s in scalar],
            out_specs=pl.BlockSpec(memory_space=pltpu.VMEM),
            out_shape=pltpu.VMEM(shape, dtype),
            **more,
        )(*(a if s else pltpu.with_memory_space_constraint(a, pltpu.VMEM) for a, s in zip(arrays, scalar)))

    return call


def attention_kernel(place, lengths, queries, own_keys, own_values, other, out):
    new_count, requests, group, dim = queries.shape
    homes, per_home = out.shape[0], new_count // out.shape[0]
    span = own_keys.shape[1]
    rows = new_count * group
    far = homes // NEAR
    kept = per_home * requests
    scale = 1.0 / math.sqrt(dim)
    head = pl.ds(pl.multiple_of(place[0] * dim, dim), dim)
    lane = lax.broadcasted_iota(jnp.int32, (homes, group, dim), 2)
    stats = jnp.zeros((homes, group, dim), f32)
    home = lax.broadcasted_iota(jnp.int32, (rows, span), 0) // (group * per_home)
    token = (home % far * NEAR + home // far) * per_home
    token += lax.broadcasted_iota(jnp.int32, (rows, span), 0) // group % per_home
    column = lax.broadcasted_iota(jnp.int32, (rows, span), 1)
    for r in range(requests):
        q = queries[:, r].astype(f32).reshape(rows, dim).astype(bf16)
        last = lengths[r] - new_count
        keys = (own_keys[r, :, head], other[pl.ds(r * span, span), :])
        values = (own_values[r, :, head], other[pl.ds((requests + r) * span, span), :])
        scores, seen = [], []
        top = None
        for part in range(2):
            s = lax.dot_general(q, keys[part], (((1,), (1,)), ((), ())), preferred_element_type=f32) * scale
            visible = column - token <= last - place[1 + part]
            s = jnp.where(visible, s, masked_fill_value)
            m = jnp.max(s, axis=1, keepdims=True)
            top = m if top is None else jnp.maximum(top, m)
            scores.append(s)
            seen.append(visible)
        shift = top.astype(bf16).astype(f32)
        total, summed = None, None
        for part in range(2):
            w = jnp.where(seen[part], jnp.exp(scores[part] - shift), 0.0)
            t = jnp.sum(w, axis=1, keepdims=True)
            o = jnp.dot(w.astype(bf16), values[part], preferred_element_type=f32)
            total = t if total is None else total + t
            summed = o if summed is None else summed + o
        high = total.astype(bf16).astype(f32)
        low = total - high
        summed = summed.reshape(homes, per_home, group, dim)
        for t in range(per_home):
            k = t * requests + r
            out[:, k] = summed[:, t].astype(bf16)
            for j, v in enumerate((shift, high, low)):
                v = v.reshape(homes, per_home, group, 1)[:, t]
                stats = jnp.where(lane == j * kept + k, v, stats)
    out[:, kept] = stats.astype(bf16)


def merged(parts):
    kept, dim = parts.shape[-3] - 1, parts.shape[-1]
    stats = parts[..., kept, :, :].astype(f32)
    shift = jnp.max(stats, axis=0)
    factor = jnp.exp(stats - shift[None])
    flat = stats.reshape(-1, dim)
    total = pltpu.roll(flat, dim - kept, 1) + pltpu.roll(flat, dim - 2 * kept, 1)
    total = jnp.sum(factor * total.reshape(stats.shape), axis=0)
    rows = [
        jnp.sum(parts[..., k, :, :].astype(f32) * factor[..., k : k + 1], axis=0) for k in range(kept)
    ]
    return rows, shift, total


def merge_near_kernel(parts, out):
    kept, dim = parts.shape[-3] - 1, parts.shape[-1]
    rows, shift, total = merged(parts)
    for k in range(kept):
        out[:, k] = rows[k].astype(bf16)
    high = total.astype(bf16).astype(f32)
    low = (total - high).reshape(-1, dim)
    high = pltpu.roll(high.reshape(-1, dim), kept, 1).reshape(shift.shape)
    low = pltpu.roll(low, 2 * kept, 1).reshape(shift.shape)
    lane = lax.broadcasted_iota(jnp.int32, shift.shape, len(shift.shape) - 1)
    out[:, kept] = jnp.where(lane < kept, shift, jnp.where(lane < 2 * kept, high, low)).astype(bf16)


def merge_far_kernel(parts, out):
    rows, _, total = merged(parts)
    for k, row in enumerate(rows):
        out[k] = (row / total[:, k : k + 1]).astype(bf16)


def project_kernel(block, place, attention, weight, other, out, wide):
    pieces, per_piece, _ = out.shape
    inputs, dim = weight.shape[0] // CORES, attention.shape[1]
    group = inputs // dim
    rows = attention.shape[0] // group
    homes = wide.shape[0] // block
    for h in range(homes):
        source = h % NEAR * (homes // NEAR) + h // NEAR
        wide[h * block : (h + 1) * block] = attention[source * block : (source + 1) * block].astype(f32)
    left = jnp.concatenate(
        [wide[pl.ds(h, rows, stride=group), :].astype(bf16) for h in range(group)], axis=1
    )
    mine = weight[pl.ds(pl.multiple_of(place[0] * inputs, inputs), inputs), :]
    theirs = other[other.shape[0] - inputs :, :]
    for right, core in ((mine, place[0]), (theirs, 1 - place[0])):
        terms = jnp.dot(left, right, preferred_element_type=f32)
        for x in range(pieces // CORES):
            out[x * CORES + core] = terms[x * per_piece : (x + 1) * per_piece]


def exchanged(pieces, axes):
    flat = pieces.reshape(pieces.shape[0], -1, pieces.shape[-1])
    return lax.all_to_all(flat, axes, 0, 0, tiled=True).reshape(pieces.shape)


def shared(value, axis):
    return exchanged(jnp.broadcast_to(value[None], (lax.axis_size(axis), *value.shape)), axis)


def body(queries, stored_cache_keys, stored_cache_values, out_weight, lengths):
    requests, span, _ = stored_cache_keys.shape
    far_count, x_count = lax.axis_size("far"), lax.axis_size("head")
    z_count = far_count * NEAR
    new_count = queries.shape[1] * z_count * CORES
    dim = HEAD_DIMENSION
    group = queries.shape[2] // (CORES * dim)
    inputs = out_weight.shape[0] // CORES
    columns = out_weight.shape[1]
    z, core = lax.axis_index(("far", "near")), lax.axis_index("core")
    per_home = new_count // z_count
    kept = per_home * requests

    def head_of(cache, which):
        return lax.dynamic_slice_in_dim(cache, which * dim, dim, 2).reshape(requests * span, dim)

    leaving = jnp.concatenate(
        [
            head_of(stored_cache_keys, 1 - core),
            head_of(stored_cache_values, 1 - core),
            lax.dynamic_slice_in_dim(out_weight, (1 - core) * inputs, inputs, 0),
        ],
        axis=0,
    )
    arrived = lax.ppermute(leaving, "core", [(0, 1), (1, 0)])

    place = jnp.stack([core, (z * CORES + core) * span, (z * CORES + 1 - core) * span]).astype(jnp.int32)
    pieces = queries.reshape(requests, CORES, group, dim).transpose(1, 0, 2, 3)
    pieces = jnp.broadcast_to(pieces[None], (far_count, *pieces.shape)).reshape(-1, *pieces.shape[1:])
    some_queries = exchanged(pieces, ("far", "core"))
    some_queries, arrived, place = lax.optimization_barrier((some_queries, arrived, place))
    all_queries = shared(some_queries, "near").reshape(new_count, requests, group, dim)


    partial = in_vmem(attention_kernel, (z_count, kept + 1, group, dim), bf16)(
        place, lengths, all_queries, stored_cache_keys, stored_cache_values, arrived
    )

    sent = partial.reshape(NEAR, far_count, *partial.shape[1:])
    partial = in_vmem(merge_near_kernel, sent.shape[1:], bf16)(exchanged(sent, "near"))
    own = in_vmem(merge_far_kernel, (kept, group, dim), bf16)(exchanged(partial, "far"))
    attention = lax.all_gather(own.reshape(-1, dim), "far", axis=0, tiled=True)
    attention = lax.all_gather(attention, "near", axis=0, tiled=True)

    rows = z_count * kept
    terms = in_vmem(
        functools.partial(project_kernel, kept * group),
        (x_count * CORES, rows // x_count, columns),
        f32,
        scratch_shapes=[pltpu.VMEM((rows * group, dim), f32)],
    )(place, attention.reshape(rows * group, dim), out_weight, arrived)
    terms = lax.all_to_all(terms, ("head", "core"), 0, 0, tiled=True).sum(axis=0)
    terms = terms.reshape(-1, requests, columns).transpose(1, 0, 2)
    return terms.astype(bf16)


def solution(mesh):
    shape = mesh.devices.shape
    torus = Mesh(
        mesh.devices.reshape(shape[0], -1, NEAR, CORES, shape[2]),
        ("groups", "far", "near", "core", "head"),
    )
    return jax.shard_map(
        body,
        mesh=torus,
        in_specs=(
            P("groups", BLK, "head"),
            P("groups", BLK, "head"),
            P("groups", BLK, "head"),
            P("head", BLK),
            P("groups"),
        ),
        out_specs=P("groups", "head", BLK),
        check_vma=False,
    )
```

```python
import functools
import math

import jax
import jax.numpy as jnp
from jax import lax
from jax.experimental import pallas as pl
from jax.experimental.pallas import tpu as pltpu
from jax.sharding import Mesh
from jax.sharding import PartitionSpec as P


HEAD_DIMENSION = 128
CORES = 2
BLK = ("far", "near", "core")
NEAR = 2

masked_fill_value = -1e30
bf16 = jnp.bfloat16
f32 = jnp.float32


def in_vmem(kernel, shape, dtype, **more):
    def call(*arrays):
        scalar = [a.dtype == jnp.int32 for a in arrays]
        return pl.pallas_call(
            kernel,
            in_specs=[pl.BlockSpec(memory_space=pltpu.SMEM if s else pltpu.VMEM) for s in scalar],
            out_specs=pl.BlockSpec(memory_space=pltpu.VMEM),
            out_shape=pltpu.VMEM(shape, dtype),
            **more,
        )(*(a if s else pltpu.with_memory_space_constraint(a, pltpu.VMEM) for a, s in zip(arrays, scalar)))

    return call


def spread_kernel(queries, out):
    requests, dim = queries.shape[0], out.shape[2]
    group = out.shape[1] // requests
    wide = queries[...].astype(f32)
    for core in range(CORES):
        rows = [
            wide[r : r + 1, (core * group + h) * dim : (core * group + h + 1) * dim]
            for r in range(requests)
            for h in range(group)
        ]
        piece = jnp.concatenate(rows, axis=0).astype(bf16)
        for p in range(core, out.shape[0], CORES):
            out[p] = piece


def attention_kernel(place, lengths, queries, own_keys, own_values, other, out):
    new_count, requests, group, dim = queries.shape
    homes, per_home = out.shape[0], new_count // out.shape[0]
    span = own_keys.shape[1]
    rows = new_count * group
    far = homes // NEAR
    kept = per_home * requests
    scale = 1.0 / math.sqrt(dim)
    head = pl.ds(pl.multiple_of(place[0] * dim, dim), dim)
    lane = lax.broadcasted_iota(jnp.int32, (homes, group, dim), 2)
    stats = jnp.zeros((homes, group, dim), f32)
    home = lax.broadcasted_iota(jnp.int32, (rows, span), 0) // (group * per_home)
    token = (home % far * NEAR + home // far) * per_home
    token += lax.broadcasted_iota(jnp.int32, (rows, span), 0) // group % per_home
    column = lax.broadcasted_iota(jnp.int32, (rows, span), 1)
    for r in range(requests):
        q = queries[:, r].astype(f32).reshape(rows, dim).astype(bf16)
        last = lengths[r] - new_count
        keys = (own_keys[r, :, head], other[pl.ds(r * span, span), :])
        values = (own_values[r, :, head], other[pl.ds((requests + r) * span, span), :])
        scores = []
        for part in range(2):
            s = lax.dot_general(q, keys[part], (((1,), (1,)), ((), ())), preferred_element_type=f32)
            visible = column - token <= last - place[1 + part]
            scores.append(jnp.where(visible, s * scale, masked_fill_value))
        shift = jnp.max(jnp.maximum(*scores), axis=1, keepdims=True).astype(bf16).astype(f32)
        lowest = jnp.maximum(shift, 0.1 * masked_fill_value)
        weights = [jnp.exp(s - lowest) for s in scores]
        total = jnp.sum(weights[0] + weights[1], axis=1, keepdims=True)
        summed = sum(
            jnp.dot(w.astype(bf16), v, preferred_element_type=f32) for w, v in zip(weights, values)
        )
        high = total.astype(bf16).astype(f32)
        low = total - high
        summed = summed.reshape(homes, per_home, group, dim)
        for t in range(per_home):
            k = t * requests + r
            out[:, k] = summed[:, t].astype(bf16)
            for j, v in enumerate((shift, high, low)):
                v = v.reshape(homes, per_home, group, 1)[:, t]
                stats = jnp.where(lane == j * kept + k, v, stats)
    out[:, kept] = stats.astype(bf16)


def merged(parts):
    kept, dim = parts.shape[-3] - 1, parts.shape[-1]
    stats = parts[..., kept, :, :].astype(f32)
    shift = jnp.max(stats, axis=0)
    factor = jnp.exp(stats - shift[None])
    flat = stats.reshape(-1, dim)
    total = pltpu.roll(flat, dim - kept, 1) + pltpu.roll(flat, dim - 2 * kept, 1)
    total = jnp.sum(factor * total.reshape(stats.shape), axis=0)
    rows = [
        jnp.sum(parts[..., k, :, :].astype(f32) * factor[..., k : k + 1], axis=0) for k in range(kept)
    ]
    return rows, shift, total


def merge_near_kernel(parts, out):
    kept, dim = parts.shape[-3] - 1, parts.shape[-1]
    rows, shift, total = merged(parts)
    for k in range(kept):
        out[:, k] = rows[k].astype(bf16)
    high = total.astype(bf16).astype(f32)
    low = (total - high).reshape(-1, dim)
    high = pltpu.roll(high.reshape(-1, dim), kept, 1).reshape(shift.shape)
    low = pltpu.roll(low, 2 * kept, 1).reshape(shift.shape)
    lane = lax.broadcasted_iota(jnp.int32, shift.shape, len(shift.shape) - 1)
    out[:, kept] = jnp.where(lane < kept, shift, jnp.where(lane < 2 * kept, high, low)).astype(bf16)


def merge_far_kernel(parts, out):
    rows, _, total = merged(parts)
    for k, row in enumerate(rows):
        row = (row / total[:, k : k + 1]).astype(bf16)
        out[:, k] = jnp.broadcast_to(row[None], (out.shape[0], *row.shape))


def project_kernel(block, place, attention, weight, other, out, wide):
    pieces, per_piece, _ = out.shape
    inputs, dim = weight.shape[0] // CORES, attention.shape[1]
    group = inputs // dim
    rows = attention.shape[0] // group
    homes = wide.shape[0] // block
    for h in range(homes):
        source = h % NEAR * (homes // NEAR) + h // NEAR
        wide[h * block : (h + 1) * block] = attention[source * block : (source + 1) * block].astype(f32)
    left = jnp.concatenate(
        [wide[pl.ds(h, rows, stride=group), :].astype(bf16) for h in range(group)], axis=1
    )
    mine = weight[pl.ds(pl.multiple_of(place[0] * inputs, inputs), inputs), :]
    theirs = other[other.shape[0] - inputs :, :]
    for right, core in ((mine, place[0]), (theirs, 1 - place[0])):
        terms = jnp.dot(left, right, preferred_element_type=f32)
        for x in range(pieces // CORES):
            out[x * CORES + core] = terms[x * per_piece : (x + 1) * per_piece]


def exchanged(pieces, axes):
    flat = pieces.reshape(pieces.shape[0], -1, pieces.shape[-1])
    return lax.all_to_all(flat, axes, 0, 0, tiled=True).reshape(pieces.shape)


def shared(value, axis):
    return exchanged(jnp.broadcast_to(value[None], (lax.axis_size(axis), *value.shape)), axis)


def body(queries, stored_cache_keys, stored_cache_values, out_weight, lengths):
    requests, span, _ = stored_cache_keys.shape
    far_count, x_count = lax.axis_size("far"), lax.axis_size("head")
    z_count = far_count * NEAR
    new_count = queries.shape[1] * z_count * CORES
    dim = HEAD_DIMENSION
    group = queries.shape[2] // (CORES * dim)
    inputs = out_weight.shape[0] // CORES
    columns = out_weight.shape[1]
    z, core = lax.axis_index(("far", "near")), lax.axis_index("core")
    per_home = new_count // z_count
    kept = per_home * requests

    def head_of(cache, which):
        return lax.dynamic_slice_in_dim(cache, which * dim, dim, 2).reshape(requests * span, dim)

    leaving = jnp.concatenate(
        [
            head_of(stored_cache_keys, 1 - core),
            head_of(stored_cache_values, 1 - core),
            lax.dynamic_slice_in_dim(out_weight, (1 - core) * inputs, inputs, 0),
        ],
        axis=0,
    )
    arrived = lax.ppermute(leaving, "core", [(0, 1), (1, 0)])

    place = jnp.stack([core, (z * CORES + core) * span, (z * CORES + 1 - core) * span]).astype(jnp.int32)
    pieces = in_vmem(spread_kernel, (far_count * CORES, requests * group, dim), bf16)(queries.reshape(requests, -1))
    some_queries = lax.all_to_all(pieces, ("far", "core"), 0, 0, tiled=True)
    some_queries, arrived, place = lax.optimization_barrier((some_queries, arrived, place))
    all_queries = shared(some_queries, "near").reshape(new_count, requests, group, dim)


    partial = in_vmem(attention_kernel, (z_count, kept + 1, group, dim), bf16)(
        place, lengths, all_queries, stored_cache_keys, stored_cache_values, arrived
    )

    sent = partial.reshape(NEAR, far_count, *partial.shape[1:])
    partial = in_vmem(merge_near_kernel, sent.shape[1:], bf16)(exchanged(sent, "near"))
    own = in_vmem(merge_far_kernel, (far_count, kept, group, dim), bf16)(
        exchanged(partial, "far")
    )
    attention = shared(exchanged(own, "far"), "near")

    rows = z_count * kept
    terms = in_vmem(
        functools.partial(project_kernel, kept * group),
        (x_count * CORES, rows // x_count, columns),
        f32,
        scratch_shapes=[pltpu.VMEM((rows * group, dim), f32)],
    )(place, attention.reshape(rows * group, dim), out_weight, arrived)
    terms = lax.all_to_all(terms, ("head", "core"), 0, 0, tiled=True).sum(axis=0)
    terms = terms.reshape(-1, requests, columns).transpose(1, 0, 2)
    return terms.astype(bf16)


def solution(mesh):
    shape = mesh.devices.shape
    torus = Mesh(
        mesh.devices.reshape(shape[0], -1, NEAR, CORES, shape[2]),
        ("groups", "far", "near", "core", "head"),
    )
    return jax.shard_map(
        body,
        mesh=torus,
        in_specs=(
            P("groups", BLK, "head"),
            P("groups", BLK, "head"),
            P("groups", BLK, "head"),
            P("head", BLK),
            P("groups"),
        ),
        out_specs=P("groups", "head", BLK),
        check_vma=False,
    )
```

```python
import functools
import math

import jax
import jax.numpy as jnp
from jax import lax
from jax.experimental import pallas as pl
from jax.experimental.pallas import tpu as pltpu
from jax.sharding import Mesh
from jax.sharding import PartitionSpec as P


HEAD_DIMENSION = 128
CORES = 2
REQUESTS = 2
HALVES = 2
NEAR = HALVES * REQUESTS
NEAR_AXES = ("half", "req")
BLK = ("far", "half", "req", "core")

masked_fill_value = -1e30
bf16 = jnp.bfloat16
f32 = jnp.float32


def in_vmem(kernel, shape, dtype, **more):
    def call(*arrays):
        scalar = [a.dtype == jnp.int32 for a in arrays]
        return pl.pallas_call(
            kernel,
            in_specs=[pl.BlockSpec(memory_space=pltpu.SMEM if s else pltpu.VMEM) for s in scalar],
            out_specs=pl.BlockSpec(memory_space=pltpu.VMEM),
            out_shape=pltpu.VMEM(shape, dtype),
            **more,
        )(*(a if s else pltpu.with_memory_space_constraint(a, pltpu.VMEM) for a, s in zip(arrays, scalar)))

    return call


def spread_kernel(queries, out):
    requests, dim = queries.shape[0], out.shape[2]
    group = out.shape[1] // requests
    wide = queries[...].astype(f32)
    for core in range(CORES):
        rows = [
            wide[r : r + 1, (core * group + h) * dim : (core * group + h + 1) * dim]
            for r in range(requests)
            for h in range(group)
        ]
        piece = jnp.concatenate(rows, axis=0).astype(bf16)
        for p in range(core, out.shape[0], CORES):
            out[p] = piece


def attention_kernel(place, lengths, queries, own_keys, own_values, second, third, fourth, out):
    new_count, group, dim = queries.shape
    halves, far, kept = out.shape[0], out.shape[1], out.shape[2] - 1
    span = own_keys.shape[1]
    rows = new_count * group
    inner = NEAR // halves
    scale = 1.0 / math.sqrt(dim)
    core, request = place[0], place[1]
    head = pl.ds(pl.multiple_of(core * dim, dim), dim)
    row = lax.broadcasted_iota(jnp.int32, (rows, span), 0) // group
    token = row // CORES % far * (NEAR * CORES) + row // (far * CORES) * CORES + row % CORES
    ahead = lax.broadcasted_iota(jnp.int32, (rows, span), 1) - token
    q = queries[...].astype(f32).reshape(rows, dim).astype(bf16)
    last = lengths[request] - new_count
    keys = [own_keys[request, :, head]] + [other[:span, :] for other in (second, third, fourth)]
    values = [own_values[request, :, head]]
    values += [other[span : 2 * span, :] for other in (second, third, fourth)]
    scores = []
    for part, k in enumerate(keys):
        s = lax.dot_general(q, k, (((1,), (1,)), ((), ())), preferred_element_type=f32)
        scores.append(jnp.where(ahead <= last - place[2 + part], s * scale, masked_fill_value))
    shift = jnp.max(functools.reduce(jnp.maximum, scores), axis=1, keepdims=True)
    shift = shift.astype(bf16).astype(f32)
    lowest = jnp.maximum(shift, 0.1 * masked_fill_value)
    weights = [jnp.exp(s - lowest) for s in scores]
    total = jnp.sum(sum(weights), axis=1, keepdims=True)
    summed = sum(
        jnp.dot(w.astype(bf16), v, preferred_element_type=f32) for w, v in zip(weights, values)
    )
    high = total.astype(bf16).astype(f32)
    low = total - high
    lane = lax.broadcasted_iota(jnp.int32, (halves, far, group, dim), 3)
    stats = jnp.zeros((halves, far, group, dim), f32)
    summed = summed.reshape(halves, inner, far, CORES, group, dim)
    for k in range(kept):
        n, c = k // CORES, k % CORES
        out[:, :, k] = summed[:, n, :, c].astype(bf16)
        for j, v in enumerate((shift, high, low)):
            v = v.reshape(halves, inner, far, CORES, group, 1)[:, n, :, c]
            stats = jnp.where(lane == j * kept + k, v, stats)
    out[:, :, kept] = stats.astype(bf16)


def merged(parts):
    kept, dim = parts.shape[-3] - 1, parts.shape[-1]
    stats = parts[..., kept, :, :].astype(f32)
    shift = jnp.max(stats, axis=0)
    factor = jnp.exp(stats - shift[None])
    flat = stats.reshape(-1, dim)
    total = pltpu.roll(flat, dim - kept, 1) + pltpu.roll(flat, dim - 2 * kept, 1)
    total = jnp.sum(factor * total.reshape(stats.shape), axis=0)
    rows = [
        jnp.sum(parts[..., k, :, :].astype(f32) * factor[..., k : k + 1], axis=0) for k in range(kept)
    ]
    return rows, shift, total


def merge_near_kernel(parts, out):
    kept, dim = parts.shape[-3] - 1, parts.shape[-1]
    rows, shift, total = merged(parts)
    for k in range(kept):
        out[:, k] = rows[k].astype(bf16)
    high = total.astype(bf16).astype(f32)
    low = (total - high).reshape(-1, dim)
    high = pltpu.roll(high.reshape(-1, dim), kept, 1).reshape(shift.shape)
    low = pltpu.roll(low, 2 * kept, 1).reshape(shift.shape)
    lane = lax.broadcasted_iota(jnp.int32, shift.shape, len(shift.shape) - 1)
    out[:, kept] = jnp.where(lane < kept, shift, jnp.where(lane < 2 * kept, high, low)).astype(bf16)


def merge_far_kernel(parts, out):
    rows, _, total = merged(parts)
    for k, row in enumerate(rows):
        row = (row / total[:, k : k + 1]).astype(bf16)
        out[:, k] = jnp.broadcast_to(row[None], (out.shape[0], *row.shape))


def project_kernel(place, attention, weight, other, out, wide):
    pieces, per_piece, _ = out.shape
    inputs, dim = weight.shape[0] // CORES, attention.shape[1]
    group = inputs // dim
    rows = attention.shape[0] // group
    kept = NEAR // HALVES * CORES
    far_count = rows // (NEAR * kept)
    for source in range(rows):
        half, req = source // (REQUESTS * far_count * kept), source // (far_count * kept) % REQUESTS
        far, k = source // kept % far_count, source % kept
        z = far * NEAR + half * (NEAR // HALVES) + k // CORES
        at = (z * CORES + k % CORES) * REQUESTS + req
        wide[at * group : (at + 1) * group] = attention[source * group : (source + 1) * group].astype(f32)
    left = jnp.concatenate(
        [wide[pl.ds(h, rows, stride=group), :].astype(bf16) for h in range(group)], axis=1
    )
    mine = weight[pl.ds(pl.multiple_of(place[0] * inputs, inputs), inputs), :]
    theirs = other[other.shape[0] - inputs :, :]
    for right, core in ((mine, place[0]), (theirs, 1 - place[0])):
        terms = jnp.dot(left, right, preferred_element_type=f32)
        for x in range(pieces // CORES):
            out[x * CORES + core] = terms[x * per_piece : (x + 1) * per_piece]


def exchanged(pieces, axes):
    flat = pieces.reshape(pieces.shape[0], -1, pieces.shape[-1])
    return lax.all_to_all(flat, axes, 0, 0, tiled=True).reshape(pieces.shape)


def shared(value, axis):
    return exchanged(jnp.broadcast_to(value[None], (lax.axis_size(axis), *value.shape)), axis)


def body(queries, stored_cache_keys, stored_cache_values, out_weight, lengths):
    requests, span, _ = stored_cache_keys.shape
    far_count, x_count = lax.axis_size("far"), lax.axis_size("head")
    z_count = far_count * NEAR
    new_count = queries.shape[1] * z_count * CORES
    dim = HEAD_DIMENSION
    group = queries.shape[2] // (CORES * dim)
    inputs = out_weight.shape[0] // CORES
    columns = out_weight.shape[1]
    z, core, req = lax.axis_index(("far", *NEAR_AXES)), lax.axis_index("core"), lax.axis_index("req")
    kept = NEAR // HALVES * CORES
    rows = new_count * requests

    def caches(request, head):
        sizes = (1, span, dim)
        both = (stored_cache_keys, stored_cache_values)
        return [lax.dynamic_slice(a, (request, 0, head * dim), sizes).reshape(span, dim) for a in both]

    def swapped(arrays, flip_req, flip_core):
        pairs = [
            (r * CORES + c, (r ^ flip_req) * CORES + (c ^ flip_core))
            for r in range(REQUESTS)
            for c in range(CORES)
        ]
        return lax.ppermute(jnp.concatenate(arrays, axis=0), ("req", "core"), pairs)

    theirs = lax.dynamic_slice_in_dim(out_weight, (1 - core) * inputs, inputs, 0)
    second = swapped([*caches(req, 1 - core), theirs], 0, 1)
    third = swapped(caches(1 - req, core), 1, 0)
    fourth = swapped(caches(1 - req, 1 - core), 1, 1)

    other_z = z + 1 - 2 * req
    first = [z * CORES + core, z * CORES + 1 - core, other_z * CORES + core, other_z * CORES + 1 - core]
    place = jnp.stack([core, req, *(b * span for b in first)]).astype(jnp.int32)
    pieces = in_vmem(spread_kernel, (far_count * CORES, requests * group, dim), bf16)(queries.reshape(requests, -1))
    some_queries = lax.all_to_all(pieces, ("far", "core"), 0, 0, tiled=True)
    some_queries, second, third, fourth, place = lax.optimization_barrier(
        (some_queries, second, third, fourth, place)
    )
    pieces = some_queries.reshape(-1, requests, group, dim).transpose(1, 0, 2, 3)
    pieces = jnp.broadcast_to(pieces[None], (HALVES, *pieces.shape)).reshape(NEAR, *pieces.shape[1:])
    all_queries = exchanged(pieces, NEAR_AXES).reshape(new_count, group, dim)

    partial = in_vmem(attention_kernel, (HALVES, far_count, kept + 1, group, dim), bf16)(
        place, lengths, all_queries, stored_cache_keys, stored_cache_values, second, third, fourth
    )
    partial = in_vmem(merge_near_kernel, partial.shape[1:], bf16)(exchanged(partial, "half"))
    own = in_vmem(merge_far_kernel, (far_count, kept, group, dim), bf16)(
        exchanged(partial, "far")
    )
    attention = shared(exchanged(own, "far"), NEAR_AXES)

    terms = in_vmem(
        project_kernel,
        (x_count * CORES, rows // x_count, columns),
        f32,
        scratch_shapes=[pltpu.VMEM((rows * group, dim), f32)],
    )(place, attention.reshape(rows * group, dim), out_weight, second)
    terms = lax.all_to_all(terms, ("head", "core"), 0, 0, tiled=True).sum(axis=0)
    terms = terms.reshape(-1, requests, columns).transpose(1, 0, 2)
    return terms.astype(bf16)


def solution(mesh):
    shape = mesh.devices.shape
    torus = Mesh(
        mesh.devices.reshape(shape[0], -1, HALVES, REQUESTS, CORES, shape[2]),
        ("groups", *BLK, "head"),
    )
    return jax.shard_map(
        body,
        mesh=torus,
        in_specs=(
            P("groups", BLK, "head"),
            P("groups", BLK, "head"),
            P("groups", BLK, "head"),
            P("head", BLK),
            P("groups"),
        ),
        out_specs=P("groups", "head", BLK),
        check_vma=False,
    )
```

```python
import functools
import math

import jax
import jax.numpy as jnp
from jax import lax
from jax.experimental import pallas as pl
from jax.experimental.pallas import tpu as pltpu
from jax.sharding import Mesh
from jax.sharding import PartitionSpec as P


HEAD_DIMENSION = 128
CORES = 2
REQUESTS = 2
HALVES = 2
NEAR = HALVES * REQUESTS
NEAR_AXES = ("half", "req")
BLK = ("far", "half", "req", "core")

masked_fill_value = -1e30
bf16 = jnp.bfloat16
f32 = jnp.float32


def in_vmem(kernel, shape, dtype, **more):
    def call(*arrays):
        scalar = [a.dtype == jnp.int32 for a in arrays]
        return pl.pallas_call(
            kernel,
            in_specs=[pl.BlockSpec(memory_space=pltpu.SMEM if s else pltpu.VMEM) for s in scalar],
            out_specs=pl.BlockSpec(memory_space=pltpu.VMEM),
            out_shape=pltpu.VMEM(shape, dtype),
            **more,
        )(*(a if s else pltpu.with_memory_space_constraint(a, pltpu.VMEM) for a, s in zip(arrays, scalar)))

    return call


def spread_kernel(queries, out):
    requests, dim = queries.shape[0], out.shape[2]
    group = out.shape[1] // requests
    wide = queries[...].astype(f32)
    for core in range(CORES):
        rows = [
            wide[r : r + 1, (core * group + h) * dim : (core * group + h + 1) * dim]
            for r in range(requests)
            for h in range(group)
        ]
        piece = jnp.concatenate(rows, axis=0).astype(bf16)
        for p in range(core, out.shape[0], CORES):
            out[p] = piece


def attention_kernel(place, lengths, queries, own_keys, own_values, lent, other, out):
    new_count, group, dim = queries.shape
    halves, far, kept = out.shape[0], out.shape[1], out.shape[2] - 1
    span = own_keys.shape[1]
    rows = new_count * group
    inner = NEAR // halves
    scale = 1.0 / math.sqrt(dim)
    core, request = place[0], place[1]
    head = pl.ds(pl.multiple_of(core * dim, dim), dim)
    row = lax.broadcasted_iota(jnp.int32, (rows, span), 0) // group
    token = row // CORES % far * (NEAR * CORES) + row // (far * CORES) * CORES + row % CORES
    ahead = lax.broadcasted_iota(jnp.int32, (rows, span), 1) - token
    q = queries[...].astype(f32).reshape(rows, dim).astype(bf16)
    last = lengths[request] - new_count
    keys = [own_keys[request, :, head], other[:span, :], lent[:span, head], other[2 * span : 3 * span, :]]
    values = [own_values[request, :, head], other[span : 2 * span, :]]
    values += [lent[span:, head], other[3 * span : 4 * span, :]]
    scores = []
    for part, k in enumerate(keys):
        s = lax.dot_general(q, k, (((1,), (1,)), ((), ())), preferred_element_type=f32)
        scores.append(jnp.where(ahead <= last - place[2 + part], s * scale, masked_fill_value))
    shift = jnp.max(functools.reduce(jnp.maximum, scores), axis=1, keepdims=True)
    shift = shift.astype(bf16).astype(f32)
    lowest = jnp.maximum(shift, 0.1 * masked_fill_value)
    weights = [jnp.exp(s - lowest) for s in scores]
    total = jnp.sum(sum(weights), axis=1, keepdims=True)
    summed = sum(
        jnp.dot(w.astype(bf16), v, preferred_element_type=f32) for w, v in zip(weights, values)
    )
    high = total.astype(bf16).astype(f32)
    low = total - high
    lane = lax.broadcasted_iota(jnp.int32, (halves, far, group, dim), 3)
    stats = jnp.zeros((halves, far, group, dim), f32)
    summed = summed.reshape(halves, inner, far, CORES, group, dim)
    for k in range(kept):
        n, c = k // CORES, k % CORES
        out[:, :, k] = summed[:, n, :, c].astype(bf16)
        for j, v in enumerate((shift, high, low)):
            v = v.reshape(halves, inner, far, CORES, group, 1)[:, n, :, c]
            stats = jnp.where(lane == j * kept + k, v, stats)
    out[:, :, kept] = stats.astype(bf16)


def merged(parts):
    kept, dim = parts.shape[-3] - 1, parts.shape[-1]
    stats = parts[..., kept, :, :].astype(f32)
    shift = jnp.max(stats, axis=0)
    factor = jnp.exp(stats - shift[None])
    flat = stats.reshape(-1, dim)
    total = pltpu.roll(flat, dim - kept, 1) + pltpu.roll(flat, dim - 2 * kept, 1)
    total = jnp.sum(factor * total.reshape(stats.shape), axis=0)
    rows = [
        jnp.sum(parts[..., k, :, :].astype(f32) * factor[..., k : k + 1], axis=0) for k in range(kept)
    ]
    return rows, shift, total


def merge_near_kernel(parts, out):
    kept, dim = parts.shape[-3] - 1, parts.shape[-1]
    rows, shift, total = merged(parts)
    for k in range(kept):
        out[:, k] = rows[k].astype(bf16)
    high = total.astype(bf16).astype(f32)
    low = (total - high).reshape(-1, dim)
    high = pltpu.roll(high.reshape(-1, dim), kept, 1).reshape(shift.shape)
    low = pltpu.roll(low, 2 * kept, 1).reshape(shift.shape)
    lane = lax.broadcasted_iota(jnp.int32, shift.shape, len(shift.shape) - 1)
    out[:, kept] = jnp.where(lane < kept, shift, jnp.where(lane < 2 * kept, high, low)).astype(bf16)


def merge_far_kernel(parts, out):
    rows, _, total = merged(parts)
    for k, row in enumerate(rows):
        row = (row / total[:, k : k + 1]).astype(bf16)
        out[:, k] = jnp.broadcast_to(row[None], (out.shape[0], *row.shape))


def project_kernel(place, attention, weight, other, out, wide):
    pieces, per_piece, _ = out.shape
    inputs, dim = weight.shape[0] // CORES, attention.shape[1]
    group = inputs // dim
    rows = attention.shape[0] // group
    kept = NEAR // HALVES * CORES
    far_count = rows // (NEAR * kept)
    for source in range(rows):
        half, req = source // (REQUESTS * far_count * kept), source // (far_count * kept) % REQUESTS
        far, k = source // kept % far_count, source % kept
        z = far * NEAR + half * (NEAR // HALVES) + k // CORES
        at = (z * CORES + k % CORES) * REQUESTS + req
        wide[at * group : (at + 1) * group] = attention[source * group : (source + 1) * group].astype(f32)
    left = jnp.concatenate(
        [wide[pl.ds(h, rows, stride=group), :].astype(bf16) for h in range(group)], axis=1
    )
    mine = weight[pl.ds(pl.multiple_of(place[0] * inputs, inputs), inputs), :]
    theirs = other[other.shape[0] - inputs :, :]
    for right, core in ((mine, place[0]), (theirs, 1 - place[0])):
        terms = jnp.dot(left, right, preferred_element_type=f32)
        for x in range(pieces // CORES):
            out[x * CORES + core] = terms[x * per_piece : (x + 1) * per_piece]


def exchanged(pieces, axes):
    flat = pieces.reshape(pieces.shape[0], -1, pieces.shape[-1])
    return lax.all_to_all(flat, axes, 0, 0, tiled=True).reshape(pieces.shape)


def shared(value, axis):
    return exchanged(jnp.broadcast_to(value[None], (lax.axis_size(axis), *value.shape)), axis)


def body(queries, stored_cache_keys, stored_cache_values, out_weight, lengths):
    requests, span, _ = stored_cache_keys.shape
    far_count, x_count = lax.axis_size("far"), lax.axis_size("head")
    z_count = far_count * NEAR
    new_count = queries.shape[1] * z_count * CORES
    dim = HEAD_DIMENSION
    group = queries.shape[2] // (CORES * dim)
    inputs = out_weight.shape[0] // CORES
    columns = out_weight.shape[1]
    z, core, req = lax.axis_index(("far", *NEAR_AXES)), lax.axis_index("core"), lax.axis_index("req")
    kept = NEAR // HALVES * CORES
    rows = new_count * requests

    def of_request(cache, request):
        return lax.dynamic_index_in_dim(cache, request, 0, keepdims=False)

    def head_of(cache, head):
        return lax.dynamic_slice_in_dim(cache, head * dim, dim, 1)

    caches = (stored_cache_keys, stored_cache_values)
    leaving = jnp.concatenate([of_request(a, 1 - req) for a in caches], axis=0)
    lent = lax.ppermute(leaving, "req", [(0, 1), (1, 0)])
    theirs = lax.dynamic_slice_in_dim(out_weight, (1 - core) * inputs, inputs, 0)
    leaving = [head_of(a, 1 - core) for a in (*(of_request(a, req) for a in caches), lent)]
    other = lax.ppermute(jnp.concatenate([*leaving, theirs], axis=0), "core", [(0, 1), (1, 0)])

    other_z = z + 1 - 2 * req
    first = [z * CORES + core, z * CORES + 1 - core, other_z * CORES + core, other_z * CORES + 1 - core]
    place = jnp.stack([core, req, *(b * span for b in first)]).astype(jnp.int32)
    pieces = in_vmem(spread_kernel, (far_count * CORES, requests * group, dim), bf16)(queries.reshape(requests, -1))
    some_queries = lax.all_to_all(pieces, ("far", "core"), 0, 0, tiled=True)
    some_queries, lent, other, place = lax.optimization_barrier((some_queries, lent, other, place))
    pieces = some_queries.reshape(-1, requests, group, dim).transpose(1, 0, 2, 3)
    pieces = jnp.broadcast_to(pieces[None], (HALVES, *pieces.shape)).reshape(NEAR, *pieces.shape[1:])
    all_queries = exchanged(pieces, NEAR_AXES).reshape(new_count, group, dim)

    partial = in_vmem(attention_kernel, (HALVES, far_count, kept + 1, group, dim), bf16)(
        place, lengths, all_queries, stored_cache_keys, stored_cache_values, lent, other
    )
    partial = in_vmem(merge_near_kernel, partial.shape[1:], bf16)(exchanged(partial, "half"))
    own = in_vmem(merge_far_kernel, (far_count, kept, group, dim), bf16)(
        exchanged(partial, "far")
    )
    attention = shared(exchanged(own, "far"), NEAR_AXES)

    terms = in_vmem(
        project_kernel,
        (x_count * CORES, rows // x_count, columns),
        f32,
        scratch_shapes=[pltpu.VMEM((rows * group, dim), f32)],
    )(place, attention.reshape(rows * group, dim), out_weight, other)
    terms = lax.all_to_all(terms, ("head", "core"), 0, 0, tiled=True).sum(axis=0)
    terms = terms.reshape(-1, requests, columns).transpose(1, 0, 2)
    return terms.astype(bf16)


def solution(mesh):
    shape = mesh.devices.shape
    torus = Mesh(
        mesh.devices.reshape(shape[0], -1, HALVES, REQUESTS, CORES, shape[2]),
        ("groups", *BLK, "head"),
    )
    return jax.shard_map(
        body,
        mesh=torus,
        in_specs=(
            P("groups", BLK, "head"),
            P("groups", BLK, "head"),
            P("groups", BLK, "head"),
            P("head", BLK),
            P("groups"),
        ),
        out_specs=P("groups", "head", BLK),
        check_vma=False,
    )
```

```python
import functools
import math

import jax
import jax.numpy as jnp
from jax import lax
from jax.experimental import pallas as pl
from jax.experimental.pallas import tpu as pltpu
from jax.sharding import Mesh
from jax.sharding import PartitionSpec as P


HEAD_DIMENSION = 128
CORES = 2
REQUESTS = 2
HALVES = 2
NEAR = HALVES * REQUESTS
NEAR_AXES = ("half", "req")
BLK = ("far", "half", "req", "core")

masked_fill_value = -1e30
bf16 = jnp.bfloat16
f32 = jnp.float32


def in_vmem(kernel, shape, dtype, **more):
    def call(*arrays):
        scalar = [a.dtype == jnp.int32 for a in arrays]
        return pl.pallas_call(
            kernel,
            in_specs=[pl.BlockSpec(memory_space=pltpu.SMEM if s else pltpu.VMEM) for s in scalar],
            out_specs=pl.BlockSpec(memory_space=pltpu.VMEM),
            out_shape=pltpu.VMEM(shape, dtype),
            **more,
        )(*(a if s else pltpu.with_memory_space_constraint(a, pltpu.VMEM) for a, s in zip(arrays, scalar)))

    return call


def spread_kernel(queries, out):
    requests, dim = queries.shape[0], out.shape[2]
    group = out.shape[1] // requests
    wide = queries[...].astype(f32)
    for core in range(CORES):
        rows = [
            wide[r : r + 1, (core * group + h) * dim : (core * group + h + 1) * dim]
            for r in range(requests)
            for h in range(group)
        ]
        piece = jnp.concatenate(rows, axis=0).astype(bf16)
        for p in range(core, out.shape[0], CORES):
            out[p] = piece


def attention_kernel(place, lengths, queries, own_keys, own_values, lent, other, out):
    new_count, group, dim = queries.shape
    halves, far, kept = out.shape[0], out.shape[1], out.shape[2] - 1
    span = own_keys.shape[1]
    rows = new_count * group
    inner = NEAR // halves
    scale = 1.0 / math.sqrt(dim)
    core, request = place[0], place[1]
    head = pl.ds(pl.multiple_of(core * dim, dim), dim)
    row = lax.broadcasted_iota(jnp.int32, (rows, dim), 0) // group
    token = row // CORES % far * (NEAR * CORES) + row // (far * CORES) * CORES + row % CORES
    before = lax.broadcasted_iota(jnp.int32, (rows, dim), 1) - token
    ahead = jnp.concatenate([before + at for at in range(0, span, dim)], axis=1)
    q = queries[...].astype(f32).reshape(rows, dim).astype(bf16)
    last = lengths[request] - new_count
    keys = [own_keys[request, :, head], other[:span, :], lent[:span, head], other[2 * span : 3 * span, :]]
    values = [own_values[request, :, head], other[span : 2 * span, :]]
    values += [lent[span:, head], other[3 * span : 4 * span, :]]
    scores = []
    for part, k in enumerate(keys):
        s = lax.dot_general(q, k, (((1,), (1,)), ((), ())), preferred_element_type=f32)
        scores.append(jnp.where(ahead <= last - place[2 + part], s * scale, masked_fill_value))
    shift = jnp.max(functools.reduce(jnp.maximum, scores), axis=1, keepdims=True)
    shift = shift.astype(bf16).astype(f32)
    lowest = jnp.maximum(shift, 0.1 * masked_fill_value)
    weights = [jnp.exp(s - lowest) for s in scores]
    total = jnp.sum(sum(weights), axis=1, keepdims=True)
    summed = sum(
        jnp.dot(w.astype(bf16), v, preferred_element_type=f32) for w, v in zip(weights, values)
    )
    high = total.astype(bf16).astype(f32)
    low = total - high
    lane = lax.broadcasted_iota(jnp.int32, (halves, far, group, dim), 3)
    stats = jnp.zeros((halves, far, group, dim), f32)
    summed = summed.reshape(halves, inner, far, CORES, group, dim)
    for k in range(kept):
        n, c = k // CORES, k % CORES
        out[:, :, k] = summed[:, n, :, c].astype(bf16)
        for j, v in enumerate((shift, high, low)):
            v = v.reshape(halves, inner, far, CORES, group, 1)[:, n, :, c]
            stats = jnp.where(lane == j * kept + k, v, stats)
    out[:, :, kept] = stats.astype(bf16)


def merged(parts):
    kept, dim = parts.shape[-3] - 1, parts.shape[-1]
    stats = parts[..., kept, :, :].astype(f32)
    shift = jnp.max(stats, axis=0)
    factor = jnp.exp(stats - shift[None])
    flat = stats.reshape(-1, dim)
    total = pltpu.roll(flat, dim - kept, 1) + pltpu.roll(flat, dim - 2 * kept, 1)
    total = jnp.sum(factor * total.reshape(stats.shape), axis=0)
    rows = [
        jnp.sum(parts[..., k, :, :].astype(f32) * factor[..., k : k + 1], axis=0) for k in range(kept)
    ]
    return rows, shift, total


def merge_near_kernel(parts, out):
    kept, dim = parts.shape[-3] - 1, parts.shape[-1]
    rows, shift, total = merged(parts)
    for k in range(kept):
        out[:, k] = rows[k].astype(bf16)
    high = total.astype(bf16).astype(f32)
    low = (total - high).reshape(-1, dim)
    high = pltpu.roll(high.reshape(-1, dim), kept, 1).reshape(shift.shape)
    low = pltpu.roll(low, 2 * kept, 1).reshape(shift.shape)
    lane = lax.broadcasted_iota(jnp.int32, shift.shape, len(shift.shape) - 1)
    out[:, kept] = jnp.where(lane < kept, shift, jnp.where(lane < 2 * kept, high, low)).astype(bf16)


def merge_far_kernel(parts, out):
    rows, _, total = merged(parts)
    for k, row in enumerate(rows):
        row = (row / total[:, k : k + 1]).astype(bf16)
        out[:, k] = jnp.broadcast_to(row[None], (out.shape[0], *row.shape))


def project_kernel(place, attention, weight, other, out, wide):
    pieces, per_piece, _ = out.shape
    inputs, dim = weight.shape[0] // CORES, attention.shape[1]
    group = inputs // dim
    rows = attention.shape[0] // group
    kept = NEAR // HALVES * CORES
    far_count = rows // (NEAR * kept)
    for source in range(rows):
        half, req = source // (REQUESTS * far_count * kept), source // (far_count * kept) % REQUESTS
        far, k = source // kept % far_count, source % kept
        z = far * NEAR + half * (NEAR // HALVES) + k // CORES
        at = (z * CORES + k % CORES) * REQUESTS + req
        wide[at * group : (at + 1) * group] = attention[source * group : (source + 1) * group].astype(f32)
    left = jnp.concatenate(
        [wide[pl.ds(h, rows, stride=group), :].astype(bf16) for h in range(group)], axis=1
    )
    mine = weight[pl.ds(pl.multiple_of(place[0] * inputs, inputs), inputs), :]
    theirs = other[other.shape[0] - inputs :, :]
    for right, core in ((mine, place[0]), (theirs, 1 - place[0])):
        terms = jnp.dot(left, right, preferred_element_type=f32)
        for x in range(pieces // CORES):
            out[x * CORES + core] = terms[x * per_piece : (x + 1) * per_piece]


def exchanged(pieces, axes):
    flat = pieces.reshape(pieces.shape[0], -1, pieces.shape[-1])
    return lax.all_to_all(flat, axes, 0, 0, tiled=True).reshape(pieces.shape)


def shared(value, axis):
    return exchanged(jnp.broadcast_to(value[None], (lax.axis_size(axis), *value.shape)), axis)


def body(queries, stored_cache_keys, stored_cache_values, out_weight, lengths):
    requests, span, _ = stored_cache_keys.shape
    far_count, x_count = lax.axis_size("far"), lax.axis_size("head")
    z_count = far_count * NEAR
    new_count = queries.shape[1] * z_count * CORES
    dim = HEAD_DIMENSION
    group = queries.shape[2] // (CORES * dim)
    inputs = out_weight.shape[0] // CORES
    columns = out_weight.shape[1]
    z, core, req = lax.axis_index(("far", *NEAR_AXES)), lax.axis_index("core"), lax.axis_index("req")
    kept = NEAR // HALVES * CORES
    rows = new_count * requests

    def of_request(cache, request):
        return lax.dynamic_index_in_dim(cache, request, 0, keepdims=False)

    def head_of(cache, head):
        return lax.dynamic_slice_in_dim(cache, head * dim, dim, 1)

    caches = (stored_cache_keys, stored_cache_values)
    leaving = jnp.concatenate([of_request(a, 1 - req) for a in caches], axis=0)
    lent = lax.ppermute(leaving, "req", [(0, 1), (1, 0)])
    theirs = lax.dynamic_slice_in_dim(out_weight, (1 - core) * inputs, inputs, 0)
    leaving = [head_of(a, 1 - core) for a in (*(of_request(a, req) for a in caches), lent)]
    other = lax.ppermute(jnp.concatenate([*leaving, theirs], axis=0), "core", [(0, 1), (1, 0)])

    other_z = z + 1 - 2 * req
    first = [z * CORES + core, z * CORES + 1 - core, other_z * CORES + core, other_z * CORES + 1 - core]
    place = jnp.stack([core, req, *(b * span for b in first)]).astype(jnp.int32)
    pieces = in_vmem(spread_kernel, (far_count * CORES, requests * group, dim), bf16)(queries.reshape(requests, -1))
    some_queries = lax.all_to_all(pieces, ("far", "core"), 0, 0, tiled=True)
    some_queries, lent, other, place = lax.optimization_barrier((some_queries, lent, other, place))
    pieces = some_queries.reshape(-1, requests, group, dim).transpose(1, 0, 2, 3)
    pieces = jnp.broadcast_to(pieces[None], (HALVES, *pieces.shape)).reshape(NEAR, *pieces.shape[1:])
    all_queries = exchanged(pieces, NEAR_AXES).reshape(new_count, group, dim)

    partial = in_vmem(attention_kernel, (HALVES, far_count, kept + 1, group, dim), bf16)(
        place, lengths, all_queries, stored_cache_keys, stored_cache_values, lent, other
    )
    partial = in_vmem(merge_near_kernel, partial.shape[1:], bf16)(exchanged(partial, "half"))
    own = in_vmem(merge_far_kernel, (far_count, kept, group, dim), bf16)(
        exchanged(partial, "far")
    )
    attention = shared(exchanged(own, "far"), NEAR_AXES)

    terms = in_vmem(
        project_kernel,
        (x_count * CORES, rows // x_count, columns),
        f32,
        scratch_shapes=[pltpu.VMEM((rows * group, dim), f32)],
    )(place, attention.reshape(rows * group, dim), out_weight, other)
    terms = lax.all_to_all(terms, ("head", "core"), 0, 0, tiled=True).sum(axis=0)
    terms = terms.reshape(-1, requests, columns).transpose(1, 0, 2)
    return terms.astype(bf16)


def solution(mesh):
    shape = mesh.devices.shape
    torus = Mesh(
        mesh.devices.reshape(shape[0], -1, HALVES, REQUESTS, CORES, shape[2]),
        ("groups", *BLK, "head"),
    )
    return jax.shard_map(
        body,
        mesh=torus,
        in_specs=(
            P("groups", BLK, "head"),
            P("groups", BLK, "head"),
            P("groups", BLK, "head"),
            P("head", BLK),
            P("groups"),
        ),
        out_specs=P("groups", "head", BLK),
        check_vma=False,
    )
```

```python
import functools
import math

import jax
import jax.numpy as jnp
from jax import lax
from jax.experimental import pallas as pl
from jax.experimental.pallas import tpu as pltpu
from jax.sharding import Mesh
from jax.sharding import PartitionSpec as P


HEAD_DIMENSION = 128
CORES = 2
REQUESTS = 2
HALVES = 2
NEAR = HALVES * REQUESTS
NEAR_AXES = ("half", "req")
BLK = ("far", "half", "req", "core")

masked_fill_value = -1e30
bf16 = jnp.bfloat16
f32 = jnp.float32


def in_vmem(kernel, shape, dtype, **more):
    def call(*arrays):
        scalar = [a.dtype == jnp.int32 for a in arrays]
        return pl.pallas_call(
            kernel,
            in_specs=[pl.BlockSpec(memory_space=pltpu.SMEM if s else pltpu.VMEM) for s in scalar],
            out_specs=pl.BlockSpec(memory_space=pltpu.VMEM),
            out_shape=pltpu.VMEM(shape, dtype),
            **more,
        )(*(a if s else pltpu.with_memory_space_constraint(a, pltpu.VMEM) for a, s in zip(arrays, scalar)))

    return call


def spread_kernel(queries, out):
    requests, dim = queries.shape[0], out.shape[2]
    group = out.shape[1] // requests
    wide = queries[...].astype(f32)
    for core in range(CORES):
        rows = [
            wide[r : r + 1, (core * group + h) * dim : (core * group + h + 1) * dim]
            for r in range(requests)
            for h in range(group)
        ]
        piece = jnp.concatenate(rows, axis=0).astype(bf16)
        for p in range(core, out.shape[0], CORES):
            out[p] = piece


def attention_kernel(lengths, queries, own_keys, own_values, lent, other, out):
    new_count, group, dim = queries.shape
    halves, far, kept = out.shape[0], out.shape[1], out.shape[2] - 1
    span = own_keys.shape[1]
    rows = new_count * group
    inner = NEAR // halves
    scale = 1.0 / math.sqrt(dim)
    core, request = lax.axis_index("core"), lax.axis_index("req")
    z = lax.axis_index("far") * NEAR + lax.axis_index("half") * REQUESTS + request
    blocks = [(a * CORES + c) * span for a in (z, z + 1 - 2 * request) for c in (core, 1 - core)]
    head = pl.ds(pl.multiple_of(core * dim, dim), dim)
    row = lax.broadcasted_iota(jnp.int32, (rows, dim), 0) // group
    token = row // CORES % far * (NEAR * CORES) + row // (far * CORES) * CORES + row % CORES
    before = lax.broadcasted_iota(jnp.int32, (rows, dim), 1) - token
    ahead = jnp.concatenate([before + at for at in range(0, span, dim)], axis=1)
    q = queries[...].astype(f32).reshape(rows, dim).astype(bf16)
    last = lengths[request] - new_count
    keys = [own_keys[request, :, head], other[:span, :], lent[:span, head], other[2 * span : 3 * span, :]]
    values = [own_values[request, :, head], other[span : 2 * span, :]]
    values += [lent[span:, head], other[3 * span : 4 * span, :]]
    scores = []
    for part, k in enumerate(keys):
        s = lax.dot_general(q, k, (((1,), (1,)), ((), ())), preferred_element_type=f32)
        scores.append(jnp.where(ahead <= last - blocks[part], s * scale, masked_fill_value))
    shift = jnp.max(functools.reduce(jnp.maximum, scores), axis=1, keepdims=True)
    shift = shift.astype(bf16).astype(f32)
    lowest = jnp.maximum(shift, 0.1 * masked_fill_value)
    weights = [jnp.exp(s - lowest) for s in scores]
    total = jnp.sum(sum(weights), axis=1, keepdims=True)
    summed = sum(
        jnp.dot(w.astype(bf16), v, preferred_element_type=f32) for w, v in zip(weights, values)
    )
    high = total.astype(bf16).astype(f32)
    low = total - high
    lane = lax.broadcasted_iota(jnp.int32, (halves, far, group, dim), 3)
    stats = jnp.zeros((halves, far, group, dim), f32)
    summed = summed.reshape(halves, inner, far, CORES, group, dim)
    for k in range(kept):
        n, c = k // CORES, k % CORES
        out[:, :, k] = summed[:, n, :, c].astype(bf16)
        for j, v in enumerate((shift, high, low)):
            v = v.reshape(halves, inner, far, CORES, group, 1)[:, n, :, c]
            stats = jnp.where(lane == j * kept + k, v, stats)
    out[:, :, kept] = stats.astype(bf16)


def merged(parts):
    kept, dim = parts.shape[-3] - 1, parts.shape[-1]
    stats = parts[..., kept, :, :].astype(f32)
    shift = jnp.max(stats, axis=0)
    factor = jnp.exp(stats - shift[None])
    flat = stats.reshape(-1, dim)
    total = pltpu.roll(flat, dim - kept, 1) + pltpu.roll(flat, dim - 2 * kept, 1)
    total = jnp.sum(factor * total.reshape(stats.shape), axis=0)
    rows = [
        jnp.sum(parts[..., k, :, :].astype(f32) * factor[..., k : k + 1], axis=0) for k in range(kept)
    ]
    return rows, shift, total


def merge_near_kernel(parts, out):
    kept, dim = parts.shape[-3] - 1, parts.shape[-1]
    rows, shift, total = merged(parts)
    for k in range(kept):
        out[:, k] = rows[k].astype(bf16)
    high = total.astype(bf16).astype(f32)
    low = (total - high).reshape(-1, dim)
    high = pltpu.roll(high.reshape(-1, dim), kept, 1).reshape(shift.shape)
    low = pltpu.roll(low, 2 * kept, 1).reshape(shift.shape)
    lane = lax.broadcasted_iota(jnp.int32, shift.shape, len(shift.shape) - 1)
    out[:, kept] = jnp.where(lane < kept, shift, jnp.where(lane < 2 * kept, high, low)).astype(bf16)


def merge_far_kernel(parts, out):
    rows, _, total = merged(parts)
    for k, row in enumerate(rows):
        row = (row / total[:, k : k + 1]).astype(bf16)
        out[:, k] = jnp.broadcast_to(row[None], (out.shape[0], *row.shape))


def project_kernel(attention, weight, other, out, wide):
    pieces, per_piece, _ = out.shape
    inputs, dim = weight.shape[0] // CORES, attention.shape[1]
    group = inputs // dim
    rows = attention.shape[0] // group
    kept = NEAR // HALVES * CORES
    far_count = rows // (NEAR * kept)
    for source in range(rows):
        half, req = source // (REQUESTS * far_count * kept), source // (far_count * kept) % REQUESTS
        far, k = source // kept % far_count, source % kept
        z = far * NEAR + half * (NEAR // HALVES) + k // CORES
        at = (z * CORES + k % CORES) * REQUESTS + req
        wide[at * group : (at + 1) * group] = attention[source * group : (source + 1) * group].astype(f32)
    left = jnp.concatenate(
        [wide[pl.ds(h, rows, stride=group), :].astype(bf16) for h in range(group)], axis=1
    )
    own_core = lax.axis_index("core")
    mine = weight[pl.ds(pl.multiple_of(own_core * inputs, inputs), inputs), :]
    theirs = other[other.shape[0] - inputs :, :]
    for right, core in ((mine, own_core), (theirs, 1 - own_core)):
        terms = jnp.dot(left, right, preferred_element_type=f32)
        for x in range(pieces // CORES):
            out[x * CORES + core] = terms[x * per_piece : (x + 1) * per_piece]


def exchanged(pieces, axes):
    flat = pieces.reshape(pieces.shape[0], -1, pieces.shape[-1])
    return lax.all_to_all(flat, axes, 0, 0, tiled=True).reshape(pieces.shape)


def shared(value, axis):
    return exchanged(jnp.broadcast_to(value[None], (lax.axis_size(axis), *value.shape)), axis)


def body(queries, stored_cache_keys, stored_cache_values, out_weight, lengths):
    requests, _, _ = stored_cache_keys.shape
    far_count, x_count = lax.axis_size("far"), lax.axis_size("head")
    z_count = far_count * NEAR
    new_count = queries.shape[1] * z_count * CORES
    dim = HEAD_DIMENSION
    group = queries.shape[2] // (CORES * dim)
    inputs = out_weight.shape[0] // CORES
    columns = out_weight.shape[1]
    core, req = lax.axis_index("core"), lax.axis_index("req")
    kept = NEAR // HALVES * CORES
    rows = new_count * requests

    def of_request(cache, request):
        return lax.dynamic_index_in_dim(cache, request, 0, keepdims=False)

    def head_of(cache, head):
        return lax.dynamic_slice_in_dim(cache, head * dim, dim, 1)

    caches = (stored_cache_keys, stored_cache_values)
    leaving = jnp.concatenate([of_request(a, 1 - req) for a in caches], axis=0)
    lent = lax.ppermute(leaving, "req", [(0, 1), (1, 0)])
    theirs = lax.dynamic_slice_in_dim(out_weight, (1 - core) * inputs, inputs, 0)
    leaving = [head_of(a, 1 - core) for a in (*(of_request(a, req) for a in caches), lent)]
    other = lax.ppermute(jnp.concatenate([*leaving, theirs], axis=0), "core", [(0, 1), (1, 0)])

    pieces = in_vmem(spread_kernel, (far_count * CORES, requests * group, dim), bf16)(queries.reshape(requests, -1))
    some_queries = lax.all_to_all(pieces, ("far", "core"), 0, 0, tiled=True)
    some_queries, lent, other = lax.optimization_barrier((some_queries, lent, other))
    pieces = some_queries.reshape(-1, requests, group, dim).transpose(1, 0, 2, 3)
    pieces = jnp.broadcast_to(pieces[None], (HALVES, *pieces.shape)).reshape(NEAR, *pieces.shape[1:])
    all_queries = exchanged(pieces, NEAR_AXES).reshape(new_count, group, dim)

    partial = in_vmem(attention_kernel, (HALVES, far_count, kept + 1, group, dim), bf16)(
        lengths, all_queries, stored_cache_keys, stored_cache_values, lent, other
    )
    partial = in_vmem(merge_near_kernel, partial.shape[1:], bf16)(exchanged(partial, "half"))
    own = in_vmem(merge_far_kernel, (far_count, kept, group, dim), bf16)(
        exchanged(partial, "far")
    )
    attention = shared(exchanged(own, "far"), NEAR_AXES)

    terms = in_vmem(
        project_kernel,
        (x_count * CORES, rows // x_count, columns),
        f32,
        scratch_shapes=[pltpu.VMEM((rows * group, dim), f32)],
    )(attention.reshape(rows * group, dim), out_weight, other)
    terms = lax.all_to_all(terms, ("head", "core"), 0, 0, tiled=True).sum(axis=0)
    terms = terms.reshape(-1, requests, columns).transpose(1, 0, 2)
    return terms.astype(bf16)


def solution(mesh):
    shape = mesh.devices.shape
    torus = Mesh(
        mesh.devices.reshape(shape[0], -1, HALVES, REQUESTS, CORES, shape[2]),
        ("groups", *BLK, "head"),
    )
    return jax.shard_map(
        body,
        mesh=torus,
        in_specs=(
            P("groups", BLK, "head"),
            P("groups", BLK, "head"),
            P("groups", BLK, "head"),
            P("head", BLK),
            P("groups"),
        ),
        out_specs=P("groups", "head", BLK),
        check_vma=False,
    )
```
